1024 devices in a mesh: gx: 16 (over y, core), gy: 16 (over z), gz: 4 (over x).
Axes of the slice: x: 4, y: 8, z: 16, core: 2. Of those that a mesh axis runs over, the one named last changes fastest.
Arguments:
- positions: float32 [3, 16, 16, 4, 512], P(None, 'gx', 'gy', 'gz'), may hold values from -6 to 6
- velocity: float32 [3, 16, 16, 4, 512], P(None, 'gx', 'gy', 'gz'), may hold values from -7.2 to 7.2
- atom_eps: float32 [16, 16, 4, 512], P('gx', 'gy', 'gz'), may hold values from 0.5 to 2
- neighbours: int32 [16, 16, 4, 32, 512], P('gx', 'gy', 'gz'), may hold values from 0 to 511
- pair_live: int32 [16, 16, 4, 32, 512], P('gx', 'gy', 'gz'), may hold values 0 or 1
- event_count: int32 [16, 16, 4], P('gx', 'gy', 'gz'), may hold values from 0 to 16, as said below
- event_atoms: int32 [16, 16, 4, 16, 128], P('gx', 'gy', 'gz'), may hold values from 0 to 2047
- event_weight: float32 [16, 16, 4, 16], P('gx', 'gy', 'gz'), may hold values from 0.2 to 1
- template_map: float32 [128, 128], replicated, may hold values from -0.5 to 0.5
Outputs:
- final_positions: float32 [3, 16, 16, 4, 512], P(None, 'gx', 'gy', 'gz')
- final_velocity: float32 [3, 16, 16, 4, 512], P(None, 'gx', 'gy', 'gz')
The draws below stay inside these ranges and needn't reach their ends.
Inputs may be any that keep to these rules, and one draw needn't show every extreme that they name: `event_count`: in every column of domains along the third dimension, the counts add up to at most 32, and one domain of the column holds 16.
All inputs are finite; a program needn't handle non-finite values. No bound on the sum of `pair_live` on one device may be relied on, other than what follows from the above.
Results may differ from the reference program's by a relative error of at most 0.0003.
Values sent between devices are 32-bit elements; how exact they have to be, the bound alone decides.
No kernel may reach another device: no remote copies, remote signals or barrier semaphores. Data moves between devices by JAX's collectives and lax.ppermute only.
A program may use at most 64 MiB of HBM per device.

```python
import math
import jax
import jax.numpy as jnp
from jax import lax

ATOMS_DEV = 512
EV_DEV = 16
NEIGH = 32
TEMPLATE = 128
FIRE_STEPS = 2
DOM_X = 16
DOM_Y = 16
DOM_Z = 4


def draw_velocity(key, part):
    shape = (3, DOM_X, DOM_Y, DOM_Z, ATOMS_DEV)
    base = jax.random.truncated_normal(key, -4.0, 4.0, shape, jnp.float32)
    domains = DOM_X * DOM_Y * DOM_Z
    ordering = jnp.arange(domains, dtype=jnp.float32).reshape(1, DOM_X, DOM_Y, DOM_Z, 1) / max(domains - 1, 1)
    scales = 0.6 * 3.0 ** ordering
    return (base * scales).astype(jnp.float32)


def fill_column(column_key):
    first_key = jax.random.fold_in(column_key, 1)
    second_key = jax.random.fold_in(column_key, 2)
    full_slot = jax.random.randint(first_key, (), 0, DOM_Z)
    cuts = jnp.sort(jax.random.randint(second_key, (DOM_Z - 1,), 0, EV_DEV + 1))
    edges = jnp.concatenate([jnp.zeros((1,), jnp.int32), cuts.astype(jnp.int32)])
    others = edges[1:] - edges[:-1]
    places = jnp.arange(DOM_Z, dtype=jnp.int32)
    lookup = jnp.clip(jnp.where(places > full_slot, places - 1, places), 0, DOM_Z - 2)
    return jnp.where(places == full_slot, EV_DEV, others[lookup]).astype(jnp.int32)


def draw_event_count(key, part):
    column_keys = jax.random.split(jax.random.fold_in(key, 3), DOM_X * DOM_Y)
    return jax.vmap(fill_column)(column_keys).reshape(DOM_X, DOM_Y, DOM_Z)


def set_ends(values, key, smallest, high):
    place = [jax.random.randint(jax.random.fold_in(key, axis), (), 0, length) for axis, length in enumerate(values.shape)]
    longest = values.shape.index(max(values.shape))
    neighbour = place[:longest] + [(place[longest] + 1) % values.shape[longest]] + place[longest + 1:]
    return values.at[tuple(place)].set(smallest).at[tuple(neighbour)].set(high)


def shard_levels(own_key, extent, cuts, smallest, largest):
    gain, own = 1.0, jax.random.fold_in(own_key, 6)
    for dim, blocks in cuts:
        draws = jnp.exp(jax.random.uniform(jax.random.fold_in(own, dim), (blocks,), jnp.float32, smallest / len(cuts), largest / len(cuts)))
        gain = gain * jnp.repeat(draws, extent[dim] // blocks).reshape([-1 if axis == dim else 1 for axis in range(len(extent))])
    return gain


def normal_values(key, shape, deviation, bound, shards=(), kind=jnp.bfloat16):
    drawn = deviation * jax.random.normal(key, shape, jnp.float32)
    if shards:
        drawn = drawn * shard_levels(key, shape, shards, -0.22, 0.18)
    return jnp.clip(drawn, -bound, bound).astype(kind)


def setup_inputs(seed: int = 0) -> dict:
    splits = jax.random.split(jax.random.key(seed), 10)
    return {
        "positions": normal_values(splits[0], (3, DOM_X, DOM_Y, DOM_Z, ATOMS_DEV), 1.0, 6.0, ((1, 16), (2, 16), (3, 4)), jnp.float32),
        "velocity": draw_velocity(jax.random.fold_in(splits[9], 71), 0),
        "atom_eps": jnp.clip(jnp.exp(math.log(2.0) - 1.3862944 * jax.random.uniform(splits[2], (DOM_X, DOM_Y, DOM_Z, ATOMS_DEV), jnp.float32) ** shard_levels(splits[2], (DOM_X, DOM_Y, DOM_Z, ATOMS_DEV), ((0, 16), (1, 16), (2, 4)), -0.2, 0.2)), 0.5, 2.0),
        "neighbours": set_ends(jax.random.randint(splits[3], (DOM_X, DOM_Y, DOM_Z, NEIGH, ATOMS_DEV), 0, ATOMS_DEV), jax.random.fold_in(splits[3], 1), 0, ATOMS_DEV - 1).astype(jnp.int32),
        "pair_live": set_ends((jax.random.randint(splits[4], (DOM_X, DOM_Y, DOM_Z, NEIGH, ATOMS_DEV), 0, 4) < 3).astype(jnp.int32), jax.random.fold_in(splits[4], 1), 0, 1),
        "event_count": draw_event_count(jax.random.fold_in(splits[9], 71), 0),
        "event_atoms": set_ends(jax.random.randint(splits[6], (DOM_X, DOM_Y, DOM_Z, EV_DEV, TEMPLATE), 0, DOM_Z * ATOMS_DEV), jax.random.fold_in(splits[6], 1), 0, (DOM_Z * ATOMS_DEV) - 1).astype(jnp.int32),
        "event_weight": jnp.clip(jnp.exp(math.log(1.0) - 1.609438 * jax.random.uniform(splits[7], (DOM_X, DOM_Y, DOM_Z, EV_DEV), jnp.float32) ** shard_levels(splits[7], (DOM_X, DOM_Y, DOM_Z, EV_DEV), ((0, 16), (1, 16), (2, 4)), -0.2, 0.2)), 0.2, 1.0),
        "template_map": normal_values(splits[8], (TEMPLATE, TEMPLATE), TEMPLATE ** -0.5, 0.5, (), jnp.float32),
    }


width_scale = 1.5
time_step = 0.1
mixing = 0.1
epsilon = 1e-06

def relax_events(group_positions, members, weights, template_map):
    gathered = jnp.take(group_positions, members, axis=1)
    centred = gathered - lax.optimization_barrier(jnp.mean(gathered, axis=2, keepdims=True))
    shifted = jnp.einsum('cnt,ts->cns', centred, template_map, precision=lax.Precision.HIGHEST)
    shifted = shifted * weights[None, :, None]
    flattened = members.reshape(-1)
    return jnp.zeros_like(group_positions).at[:, flattened].add(shifted.reshape(3, -1))

def pair_forces(neighbourhood, own_atoms, neighbour_rows, live_pairs):
    partner = jnp.take(neighbourhood, neighbour_rows, axis=1)
    separation = own_atoms[:3, None, :] - partner[:3]
    distance_sq = lax.optimization_barrier(jnp.sum(separation * separation, axis=0))
    strength = jnp.sqrt(own_atoms[3][None, :] * partner[3]) * live_pairs.astype(jnp.float32)
    strength = strength * jnp.exp(-distance_sq * (0.5 / (width_scale * width_scale))) / (width_scale * width_scale)
    return lax.optimization_barrier(jnp.sum(strength[None] * separation, axis=1))

def halo_blocks(packed, slab_index):
    pieces = []
    for offset_x in range(3):
        slab = lax.dynamic_index_in_dim(packed, (slab_index + offset_x - 1) % DOM_X, 1, False)
        for offset_y in range(3):
            for offset_z in range(3):
                pieces.append(jnp.roll(slab, (1 - offset_y, 1 - offset_z), axis=(1, 2)))
    stacked = jnp.stack(pieces, 1)
    return jnp.moveaxis(stacked, 1, 3).reshape(4, DOM_Y, DOM_Z, 27 * ATOMS_DEV)

def all_forces(moved_positions, atom_eps, neighbours, pair_live):
    packed = jnp.concatenate([moved_positions, atom_eps[None]], 0)
    offsets = (jnp.arange(NEIGH, dtype=jnp.int32) % 27 * ATOMS_DEV).astype(jnp.int32)
    rows_all = (neighbours + offsets[None, None, None, :, None]).astype(jnp.int32)

    def slab_forces(slab_index):
        neighbourhood = halo_blocks(packed, slab_index)
        own_atoms = lax.dynamic_index_in_dim(packed, slab_index, 1, False)
        neighbour_rows = lax.dynamic_index_in_dim(rows_all, slab_index, 0, False)
        live_pairs = lax.dynamic_index_in_dim(pair_live, slab_index, 0, False)
        inner = jax.vmap(pair_forces, (1, 1, 0, 0), 1)
        return jax.vmap(inner, (1, 1, 0, 0), 1)(neighbourhood, own_atoms, neighbour_rows, live_pairs)
    result = lax.map(slab_forces, jnp.arange(DOM_X, dtype=jnp.int32))
    return jnp.moveaxis(result, 0, 1)

def reference(positions, velocity, atom_eps, neighbours, pair_live, event_count, event_atoms, event_weight, template_map):
    columns = DOM_X * DOM_Y
    group_positions = jnp.moveaxis(positions.reshape(3, columns, DOM_Z * ATOMS_DEV), 1, 0)
    alive_mask = jnp.arange(EV_DEV, dtype=jnp.int32)[None, None, None, :] < event_count[..., None]
    weights = (event_weight * alive_mask.astype(event_weight.dtype)).reshape(columns, DOM_Z * EV_DEV)
    members = event_atoms.reshape(columns, DOM_Z * EV_DEV, TEMPLATE)
    displaced = jax.vmap(lambda grouped, chosen, scaled: relax_events(grouped, chosen, scaled, template_map))(group_positions, members, weights)
    moved_positions = positions + jnp.moveaxis(displaced, 0, 1).reshape(positions.shape)
    speeds = velocity
    for iteration in range(FIRE_STEPS):
        forces = all_forces(moved_positions, atom_eps, neighbours, pair_live)
        power_sum = jnp.sum(forces * speeds)
        speed_sq = jnp.sum(speeds * speeds)
        force_sq = jnp.sum(forces * forces)
        cosine = power_sum / (jnp.sqrt(speed_sq + epsilon) * jnp.sqrt(force_sq + epsilon))
        speed_ratio = jnp.sqrt((speed_sq + epsilon) / (force_sq + epsilon))
        speeds = 0.5 * (1.0 + cosine) * ((1.0 - mixing) * speeds + mixing * speed_ratio * forces)
        speeds = speeds + time_step * forces
        moved_positions = moved_positions + time_step * speeds
    return (moved_positions, speeds)
```

```python
import jax
import jax.numpy as jnp
from jax import lax
from jax.experimental import pallas as pl
from jax.experimental.pallas import tpu as pltpu
from jax.sharding import Mesh
from jax.sharding import PartitionSpec as P

EV_DEV = 16
NEIGH = 32
TEMPLATE = 128
GX = ("gx_0", "gx_1")
GXZ = ("gx_0", "gx_1", "gz")
COLUMN = 4
CHUNKS = 4
LANES = 128
F32 = jnp.float32

width_scale = 1.5
time_step = 0.1
mixing = 0.1
epsilon = 1e-06

SMEM = pl.BlockSpec(memory_space=pltpu.SMEM)
VMEM = pl.BlockSpec(memory_space=pltpu.VMEM)


def call(kernel, outs, specs, scratch=(), flops=10000):
    return pl.pallas_call(
        kernel,
        out_shape=[jax.ShapeDtypeStruct(shape, F32) for shape in outs],
        in_specs=specs,
        out_specs=[VMEM] * len(outs),
        scratch_shapes=list(scratch),
        cost_estimate=pl.CostEstimate(flops=flops, bytes_accessed=100000, transcendentals=0),
    )


def pack_kernel(count_ref, pos_ref, vel_ref, eps_ref, weight_ref, atoms_ref, out_ref):
    live = lax.broadcasted_iota(jnp.int32, (1, EV_DEV), 1) < count_ref[0, 0, 0]
    weights = jnp.where(live, weight_ref[0, 0, :, :], 0.0)
    atoms = atoms_ref[0, 0, 0, :, :].astype(F32)
    for copy in range(COLUMN):
        out_ref[copy, 24:32, :] = jnp.zeros((8, LANES), F32)
        for c in range(3):
            for q in range(CHUNKS):
                cut = pl.ds(q * LANES, LANES)
                out_ref[copy, c * 4 + q : c * 4 + q + 1, :] = pos_ref[c, 0, 0, :, cut]
                out_ref[copy, 16 + c * 4 + q : 17 + c * 4 + q, :] = vel_ref[c, 0, 0, :, cut]
        for q in range(CHUNKS):
            out_ref[copy, 12 + q : 13 + q, :] = eps_ref[0, 0, :, pl.ds(q * LANES, LANES)]
        out_ref[copy, 28:29, 0:EV_DEV] = weights
        out_ref[copy, 32:48, :] = atoms


def events_kernel(column_ref, map_ref, moved_ref, vel_ref, low_ref, high_ref, shift_ref):
    slots = COLUMN * EV_DEV
    atoms = jnp.concatenate([column_ref[z, 32:48, :] for z in range(COLUMN)], 0).astype(jnp.int32)
    low, high = atoms & (LANES - 1), atoms >> 7
    low_ref[...] = low
    high_ref[...] = high
    diagonal = lax.broadcasted_iota(jnp.int32, (EV_DEV, LANES), 0) == lax.broadcasted_iota(
        jnp.int32, (EV_DEV, LANES), 1
    )
    weights = jnp.concatenate(
        [
            jnp.sum(jnp.where(diagonal, column_ref[z, 28:29, :], 0.0), axis=1, keepdims=True)
            for z in range(COLUMN)
        ],
        0,
    )
    centred = []
    for c in range(3):
        taken = jnp.zeros((slots, LANES), F32)
        for h in range(COLUMN * CHUNKS):
            z, q = divmod(h, CHUNKS)
            row = jnp.broadcast_to(column_ref[z, c * 4 + q : c * 4 + q + 1, :], (slots, LANES))
            taken = jnp.where(high == h, jnp.take_along_axis(row, low, axis=1), taken)
        centred.append(taken - jnp.sum(taken, axis=1, keepdims=True) * (1.0 / TEMPLATE))
    shift = jnp.dot(
        jnp.concatenate(centred, 0),
        map_ref[...],
        precision=lax.Precision.HIGHEST,
        preferred_element_type=F32,
    )
    shift = shift * jnp.concatenate([weights] * 3, 0)
    for part in range(3):
        rounded = shift.astype(jnp.bfloat16).astype(F32)
        for c in range(3):
            shift_ref[part * 3 + c, :, :] = rounded[c * slots : (c + 1) * slots]
        shift = shift - rounded
    places = lax.broadcasted_iota(jnp.int32, (LANES, LANES), 0)
    rows = lax.broadcasted_iota(jnp.int32, (16, LANES), 0)

    def some_events(i, total):
        lefts, rights = [], []
        for j in range(4):
            e = pl.ds(i * 4 + j, 1)
            here = high_ref[e, :] == rows
            left = [jnp.where(here, shift_ref[n, e, :], 0.0) for n in range(9)]
            lefts.append(jnp.concatenate(left, 0).astype(jnp.bfloat16))
            rights.append(jnp.where(low_ref[e, :] == places, 1.0, 0.0).astype(jnp.bfloat16))
        return total + lax.dot_general(
            jnp.concatenate(lefts, 1),
            jnp.concatenate(rights, 1),
            (((1,), (1,)), ((), ())),
            preferred_element_type=F32,
        )

    total = lax.fori_loop(0, slots // 4, some_events, jnp.zeros((144, LANES), F32))
    displaced = total[0:48] + total[48:96] + total[96:144]
    for z in range(COLUMN):
        for c in range(3):
            there = pl.ds(c * 16 + z * 4, 4)
            moved_ref[there, :] = (
                column_ref[z, c * 4 : c * 4 + 4, :] + displaced[c * 16 + z * 4 : c * 16 + z * 4 + 4]
            )
            vel_ref[there, :] = column_ref[z, 16 + c * 4 : 20 + c * 4, :]
        moved_ref[pl.ds(48 + z * 4, 4), :] = column_ref[z, 12:16, :]


def own_forces(z, source, neigh_ref, live_ref, table_ref):
    for k in range(NEIGH):
        ab, dz = divmod(k % 27, 3)
        a, b = divmod(ab, 3)
        first = ((z + dz + 3) & 3) * 4
        for c in range(4):
            for q in range(CHUNKS):
                table_ref[c, q, k : k + 1, :] = source(a, b, c, first + q)
    forces = [[None] * CHUNKS for _ in range(3)]
    for t in range(CHUNKS):
        own = [source(1, 1, c, z * 4 + t) for c in range(4)]
        total = [jnp.zeros((8, LANES), F32)] * 3
        for g in range(NEIGH // 8):
            atoms = neigh_ref[0, 0, 0, 8 * g : 8 * g + 8, t * LANES : (t + 1) * LANES]
            live = live_ref[0, 0, 0, 8 * g : 8 * g + 8, t * LANES : (t + 1) * LANES].astype(F32)
            low, high = atoms & (LANES - 1), atoms >> 7
            taken = []
            for c in range(4):
                value = jnp.take_along_axis(table_ref[c, 0, 8 * g : 8 * g + 8, :], low, axis=1)
                for q in range(1, CHUNKS):
                    other = jnp.take_along_axis(table_ref[c, q, 8 * g : 8 * g + 8, :], low, axis=1)
                    value = jnp.where(high == q, other, value)
                taken.append(value)
            apart = [own[c] - taken[c] for c in range(3)]
            square = apart[0] * apart[0] + apart[1] * apart[1] + apart[2] * apart[2]
            strength = jnp.sqrt(own[3] * taken[3]) * live
            strength = (
                strength
                * jnp.exp(-square * (0.5 / (width_scale * width_scale)))
                * (1.0 / (width_scale * width_scale))
            )
            total = [total[c] + strength * apart[c] for c in range(3)]
        for c in range(3):
            forces[c][t] = jnp.sum(total[c], axis=0, keepdims=True)
    return forces


def three_sums(forces, speeds):
    pairs = ((forces, speeds), (speeds, speeds), (forces, forces))
    lane = lax.broadcasted_iota(jnp.int32, (1, LANES), 1)
    packed = jnp.zeros((1, LANES), F32)
    for n, (left, right) in enumerate(pairs):
        added = sum(left[c][t] * right[c][t] for c in range(3) for t in range(CHUNKS))
        packed = jnp.where(lane == n, jnp.sum(added, axis=1, keepdims=True), packed)
    return packed


def read_sums(summed):
    lane = lax.broadcasted_iota(jnp.int32, (1, LANES), 1)
    return [
        jnp.sum(jnp.where(lane == n, summed, 0.0), axis=1, keepdims=True) for n in range(3)
    ]


def mix_factors(sums):
    power_sum, speed_sq, force_sq = sums
    cosine = power_sum / (jnp.sqrt(speed_sq + epsilon) * jnp.sqrt(force_sq + epsilon))
    speed_ratio = jnp.sqrt((speed_sq + epsilon) / (force_sq + epsilon))
    return 0.5 * (1.0 + cosine), mixing * speed_ratio


def new_speed(factors, speed, force):
    scale, ratio = factors
    return scale * ((1.0 - mixing) * speed + ratio * force) + time_step * force


def first_kernel(z_ref, m_ref, o_ref, p_ref, vel_ref, neigh_ref, live_ref, out_ref, table_ref):
    z = z_ref[0]
    halo = (m_ref, o_ref, p_ref)
    source = lambda a, b, c, row: halo[a][b, pl.ds(c * 16 + row, 1), :]
    forces = own_forces(z, source, neigh_ref, live_ref, table_ref)
    speeds = [
        [vel_ref[pl.ds(c * 16 + z * 4 + t, 1), :] for t in range(CHUNKS)] for c in range(3)
    ]
    sums = three_sums(forces, speeds)
    for copy in range(COLUMN):
        for c in range(3):
            for t in range(CHUNKS):
                out_ref[copy, c * 4 + t : c * 4 + t + 1, :] = forces[c][t]
        out_ref[copy, 12:16, :] = jnp.broadcast_to(sums, (4, LANES))


def column_kernel(parts_ref, vel_ref, out_ref, sums_ref):
    for z in range(COLUMN):
        for c in range(3):
            out_ref[pl.ds(c * 16 + z * 4, 4), :] = parts_ref[z, c * 4 : c * 4 + 4, :]
    out_ref[48:96, :] = vel_ref[...]
    total = sum(parts_ref[z, 12:13, :] for z in range(COLUMN))
    for n in range(sums_ref.shape[0]):
        sums_ref[n, :, :] = total


def second_kernel(
    z_ref, m_ref, o_ref, p_ref, fm_ref, fo_ref, fp_ref, sums_ref, neigh_ref, live_ref,
    out_ref, own_sums_ref, table_ref, new_ref,
):
    z = z_ref[0]
    factors = mix_factors(read_sums(jnp.sum(sums_ref[...], axis=0)))
    halo, pushed = (m_ref, o_ref, p_ref), (fm_ref, fo_ref, fp_ref)
    for a in range(3):
        for b in range(3):
            speed = new_speed(factors, pushed[a][b, 48:96, :], pushed[a][b, 0:48, :])
            new_ref[a * 3 + b, 0:48, :] = halo[a][b, 0:48, :] + time_step * speed
            new_ref[a * 3 + b, 48:64, :] = halo[a][b, 48:64, :]
            if a == 1 and b == 1:
                new_ref[9, 0:48, :] = speed
    source = lambda a, b, c, row: new_ref[a * 3 + b, pl.ds(c * 16 + row, 1), :]
    forces = own_forces(z, source, neigh_ref, live_ref, table_ref)
    own = lambda n: [
        [new_ref[n, pl.ds(c * 16 + z * 4 + t, 1), :] for t in range(CHUNKS)] for c in range(3)
    ]
    places, speeds = own(4), own(9)
    for c in range(3):
        for t in range(CHUNKS):
            out_ref[c * 4 + t : c * 4 + t + 1, :] = places[c][t]
            out_ref[12 + c * 4 + t : 13 + c * 4 + t, :] = speeds[c][t]
            out_ref[24 + c * 4 + t : 25 + c * 4 + t, :] = forces[c][t]
    sums = three_sums(forces, speeds)
    for n in range(own_sums_ref.shape[0]):
        own_sums_ref[n, :, :] = sums


def final_kernel(own_ref, sums_ref, pos_ref, vel_ref):
    factors = mix_factors(read_sums(jnp.sum(sums_ref[...], axis=0)))
    speed = new_speed(factors, own_ref[12:24, :], own_ref[24:36, :])
    place = own_ref[0:12, :] + time_step * speed
    for c in range(3):
        for t in range(CHUNKS):
            cut = pl.ds(t * LANES, LANES)
            pos_ref[c, 0, 0, :, cut] = place[c * 4 + t : c * 4 + t + 1]
            vel_ref[c, 0, 0, :, cut] = speed[c * 4 + t : c * 4 + t + 1]


def exchanged(x, axes):
    return lax.all_to_all(x, axes, 0, 0, tiled=True)


def added_for_each(parts, count):
    return jnp.broadcast_to(jnp.sum(parts, 0, keepdims=True), (count, 1, LANES))


def both_sides(x, axis):
    size = lax.axis_size(axis)
    up = [(i, (i + 1) % size) for i in range(size)]
    before = lax.ppermute(x, axis, up)
    after = lax.ppermute(x, axis, [(j, i) for i, j in up])
    return before, after


def halo(x):
    before, after = both_sides(x, "gy")
    row = jnp.stack([before, x, after])
    before, after = both_sides(row, GX)
    return before, row, after


def shards(
    positions,
    velocity,
    atom_eps,
    neighbours,
    pair_live,
    event_count,
    event_atoms,
    event_weight,
    template_map,
):
    x_size, y_size = lax.axis_size(GX), lax.axis_size("gy")
    z = lax.axis_index("gz").astype(jnp.int32).reshape(1)
    (own,) = call(pack_kernel, [(COLUMN, 48, LANES)], [SMEM] + [VMEM] * 5)(
        event_count, positions, velocity, atom_eps, event_weight, event_atoms
    )
    column = exchanged(own, "gz")
    moved, speeds = call(
        events_kernel,
        [(64, LANES), (48, LANES)],
        [VMEM] * 2,
        [
            pltpu.VMEM((64, LANES), jnp.int32),
            pltpu.VMEM((64, LANES), jnp.int32),
            pltpu.VMEM((9, 64, LANES), F32),
        ],
    )(column, template_map)
    around = halo(moved)
    table = pltpu.VMEM((4, CHUNKS, NEIGH, LANES), F32)
    (pushed,) = call(first_kernel, [(COLUMN, 16, LANES)], [SMEM] + [VMEM] * 6, [table])(
        z, *around, speeds, neighbours, pair_live
    )
    pushed = exchanged(pushed, "gz")
    forces, sums = call(column_kernel, [(96, LANES), (x_size, 1, LANES)], [VMEM] * 2)(
        pushed, speeds
    )
    forces_around = halo(forces)
    sums = exchanged(sums, GX)
    sums = exchanged(added_for_each(sums, y_size), "gy")
    result, sums = call(
        second_kernel,
        [(40, LANES), (x_size * COLUMN, 1, LANES)],
        [SMEM] + [VMEM] * 9,
        [table, pltpu.VMEM((10, 64, LANES), F32)],
    )(z, *around, *forces_around, sums, neighbours, pair_live)
    sums = exchanged(sums, GXZ)
    sums = exchanged(added_for_each(sums, y_size), "gy")
    return tuple(
        call(final_kernel, [positions.shape, velocity.shape], [VMEM] * 2)(result, sums)
    )


def solution(mesh):
    shape = mesh.shape
    split = Mesh(
        mesh.devices.reshape(shape["gx"] // 2, 2, shape["gy"], shape["gz"]),
        ("gx_0", "gx_1", "gy", "gz"),
    )
    in_specs = (
        P(None, GX, "gy", "gz", None),
        P(None, GX, "gy", "gz", None),
        P(GX, "gy", "gz", None),
        P(GX, "gy", "gz", None, None),
        P(GX, "gy", "gz", None, None),
        P(GX, "gy", "gz"),
        P(GX, "gy", "gz", None, None),
        P(GX, "gy", "gz", None),
        P(),
    )
    out_specs = (P(None, GX, "gy", "gz", None), P(None, GX, "gy", "gz", None))
    return jax.shard_map(
        shards, mesh=split, in_specs=in_specs, out_specs=out_specs, check_vma=False
    )
```

```python
import jax
import jax.numpy as jnp
from jax import lax
from jax.experimental import pallas as pl
from jax.experimental.pallas import tpu as pltpu
from jax.sharding import Mesh
from jax.sharding import PartitionSpec as P

EV_DEV = 16
NEIGH = 32
TEMPLATE = 128
GX = ("gx_0", "gx_1")
GXZ = ("gx_0", "gx_1", "gz")
COLUMN = 4
CHUNKS = 4
LIVE = 32
LANES = 128
F32 = jnp.float32

width_scale = 1.5
time_step = 0.1
mixing = 0.1
epsilon = 1e-06

SMEM = pl.BlockSpec(memory_space=pltpu.SMEM)
VMEM = pl.BlockSpec(memory_space=pltpu.VMEM)
HBM = pl.BlockSpec(memory_space=pltpu.HBM)


def call(kernel, outs, specs, scratch=(), limit=4 << 20):
    return pl.pallas_call(
        kernel,
        out_shape=[jax.ShapeDtypeStruct(shape, F32) for shape in outs],
        in_specs=specs,
        out_specs=[VMEM] * len(outs),
        scratch_shapes=list(scratch),
        cost_estimate=pl.CostEstimate(flops=10000, bytes_accessed=100000, transcendentals=0),
        compiler_params=pltpu.CompilerParams(vmem_limit_bytes=limit),
    )


def pack_kernel(
    count_ref, pos_hbm, vel_hbm, eps_hbm, weight_hbm, atoms_hbm, out_ref,
    pos_ref, vel_ref, eps_ref, weight_ref, atoms_ref, sems,
):
    pairs = (
        (pos_hbm, pos_ref),
        (vel_hbm, vel_ref),
        (eps_hbm, eps_ref),
        (weight_hbm, weight_ref),
        (atoms_hbm, atoms_ref),
    )
    copies = [pltpu.make_async_copy(*pair, sems.at[n]) for n, pair in enumerate(pairs)]
    for copy in copies:
        copy.start()
    for copy in range(COLUMN):
        out_ref[copy, 24:32, :] = jnp.zeros((8, LANES), F32)
    for copy in copies:
        copy.wait()
    count = count_ref[0, 0, 0]
    live = lax.broadcasted_iota(jnp.int32, (1, EV_DEV), 1) < count
    weights = jnp.where(live, weight_ref[0, 0, :, :], 0.0)
    counts = jnp.full((1, LANES), count, jnp.int32).astype(F32)
    atoms = atoms_ref[0, 0, 0, :, :].astype(F32)
    for copy in range(COLUMN):
        for c in range(3):
            for q in range(CHUNKS):
                cut = pl.ds(q * LANES, LANES)
                out_ref[copy, c * 4 + q : c * 4 + q + 1, :] = pos_ref[c, 0, 0, :, cut]
                out_ref[copy, 16 + c * 4 + q : 17 + c * 4 + q, :] = vel_ref[c, 0, 0, :, cut]
        for q in range(CHUNKS):
            out_ref[copy, 12 + q : 13 + q, :] = eps_ref[0, 0, :, pl.ds(q * LANES, LANES)]
        out_ref[copy, 28:29, 0:EV_DEV] = weights
        out_ref[copy, 29:30, :] = counts
        out_ref[copy, 32:48, :] = atoms


def events_kernel(column_ref, map_ref, moved_ref, vel_ref, atoms_ref, low_ref, high_ref, shift_ref):
    atoms_ref[...] = jnp.zeros(atoms_ref.shape, F32)
    first = jnp.int32(0)
    lane_weights = jnp.zeros((1, LANES), F32)
    for z in range(COLUMN):
        for e in range(EV_DEV):
            atoms_ref[pl.ds(first + e, 1), :] = column_ref[z, 32 + e : 33 + e, :]
        lane_weights = lane_weights + pltpu.roll(column_ref[z, 28:29, :], first, 1)
        if z < COLUMN - 1:
            first = first + jnp.max(column_ref[z, 29:30, :]).astype(jnp.int32)
    atoms = atoms_ref[0:LIVE, :].astype(jnp.int32)
    low, high = atoms & (LANES - 1), atoms >> 7
    low_ref[...] = low
    high_ref[...] = high
    slot = lax.broadcasted_iota(jnp.int32, (LIVE, LANES), 0)
    lane = lax.broadcasted_iota(jnp.int32, (LIVE, LANES), 1)
    weights = jnp.sum(jnp.where(slot == lane, lane_weights, 0.0), axis=1, keepdims=True)
    centred = []
    for c in range(3):
        taken = jnp.zeros((LIVE, LANES), F32)
        for h in range(COLUMN * CHUNKS):
            z, q = divmod(h, CHUNKS)
            row = jnp.broadcast_to(column_ref[z, c * 4 + q : c * 4 + q + 1, :], (LIVE, LANES))
            taken = jnp.where(high == h, jnp.take_along_axis(row, low, axis=1), taken)
        centred.append(taken - jnp.sum(taken, axis=1, keepdims=True) * (1.0 / TEMPLATE))
    shift = jnp.dot(
        jnp.concatenate(centred, 0),
        map_ref[...],
        precision=lax.Precision.HIGHEST,
        preferred_element_type=F32,
    )
    shift = shift * jnp.concatenate([weights] * 3, 0)
    for part in range(3):
        rounded = shift.astype(jnp.bfloat16).astype(F32)
        for c in range(3):
            shift_ref[part * 3 + c, :, :] = rounded[c * LIVE : (c + 1) * LIVE]
        shift = shift - rounded
    places = lax.broadcasted_iota(jnp.int32, (LANES, LANES), 0)
    rows = lax.broadcasted_iota(jnp.int32, (16, LANES), 0)
    total = jnp.zeros((144, LANES), F32)
    for i in range(LIVE // 4):
        lefts, rights = [], []
        for j in range(4):
            e = slice(i * 4 + j, i * 4 + j + 1)
            here = high_ref[e, :] == rows
            left = [jnp.where(here, shift_ref[n, e, :], 0.0) for n in range(9)]
            lefts.append(jnp.concatenate(left, 0).astype(jnp.bfloat16))
            rights.append(jnp.where(low_ref[e, :] == places, 1.0, 0.0).astype(jnp.bfloat16))
        total = total + lax.dot_general(
            jnp.concatenate(lefts, 1),
            jnp.concatenate(rights, 1),
            (((1,), (1,)), ((), ())),
            preferred_element_type=F32,
        )
    displaced = total[0:48] + total[48:96] + total[96:144]
    for z in range(COLUMN):
        for c in range(3):
            there = pl.ds(c * 16 + z * 4, 4)
            moved_ref[there, :] = (
                column_ref[z, c * 4 : c * 4 + 4, :] + displaced[c * 16 + z * 4 : c * 16 + z * 4 + 4]
            )
            vel_ref[there, :] = column_ref[z, 16 + c * 4 : 20 + c * 4, :]
        moved_ref[pl.ds(48 + z * 4, 4), :] = column_ref[z, 12:16, :]


def own_forces(z, source, neigh_ref, live_ref, table_ref):
    for k in range(NEIGH):
        ab, dz = divmod(k % 27, 3)
        a, b = divmod(ab, 3)
        first = ((z + dz + 3) & 3) * 4
        for c in range(4):
            for q in range(CHUNKS):
                table_ref[c, q, k : k + 1, :] = source(a, b, c, first + q)
    forces = [[None] * CHUNKS for _ in range(3)]
    for t in range(CHUNKS):
        own = [source(1, 1, c, z * 4 + t) for c in range(4)]
        total = [jnp.zeros((8, LANES), F32)] * 3
        for g in range(NEIGH // 8):
            atoms = neigh_ref[0, 0, 0, 8 * g : 8 * g + 8, t * LANES : (t + 1) * LANES]
            live = live_ref[0, 0, 0, 8 * g : 8 * g + 8, t * LANES : (t + 1) * LANES].astype(F32)
            low, high = atoms & (LANES - 1), atoms >> 7
            taken = []
            for c in range(4):
                value = jnp.take_along_axis(table_ref[c, 0, 8 * g : 8 * g + 8, :], low, axis=1)
                for q in range(1, CHUNKS):
                    other = jnp.take_along_axis(table_ref[c, q, 8 * g : 8 * g + 8, :], low, axis=1)
                    value = jnp.where(high == q, other, value)
                taken.append(value)
            apart = [own[c] - taken[c] for c in range(3)]
            square = apart[0] * apart[0] + apart[1] * apart[1] + apart[2] * apart[2]
            strength = jnp.sqrt(own[3] * taken[3]) * live
            strength = (
                strength
                * jnp.exp(-square * (0.5 / (width_scale * width_scale)))
                * (1.0 / (width_scale * width_scale))
            )
            total = [total[c] + strength * apart[c] for c in range(3)]
        for c in range(3):
            forces[c][t] = jnp.sum(total[c], axis=0, keepdims=True)
    return forces


def three_sums(forces, speeds):
    pairs = ((forces, speeds), (speeds, speeds), (forces, forces))
    lane = lax.broadcasted_iota(jnp.int32, (1, LANES), 1)
    packed = jnp.zeros((1, LANES), F32)
    for n, (left, right) in enumerate(pairs):
        added = sum(left[c][t] * right[c][t] for c in range(3) for t in range(CHUNKS))
        packed = jnp.where(lane == n, jnp.sum(added, axis=1, keepdims=True), packed)
    return packed


def read_sums(summed):
    lane = lax.broadcasted_iota(jnp.int32, (1, LANES), 1)
    return [
        jnp.sum(jnp.where(lane == n, summed, 0.0), axis=1, keepdims=True) for n in range(3)
    ]


def mix_factors(sums):
    power_sum, speed_sq, force_sq = sums
    cosine = power_sum / (jnp.sqrt(speed_sq + epsilon) * jnp.sqrt(force_sq + epsilon))
    speed_ratio = jnp.sqrt((speed_sq + epsilon) / (force_sq + epsilon))
    return 0.5 * (1.0 + cosine), mixing * speed_ratio


def new_speed(factors, speed, force):
    scale, ratio = factors
    return scale * ((1.0 - mixing) * speed + ratio * force) + time_step * force


def first_kernel(z_ref, m_ref, o_ref, p_ref, vel_ref, neigh_ref, live_ref, out_ref, table_ref):
    z = z_ref[0]
    halo = (m_ref, o_ref, p_ref)
    source = lambda a, b, c, row: halo[a][b, pl.ds(c * 16 + row, 1), :]
    forces = own_forces(z, source, neigh_ref, live_ref, table_ref)
    speeds = [
        [vel_ref[pl.ds(c * 16 + z * 4 + t, 1), :] for t in range(CHUNKS)] for c in range(3)
    ]
    sums = three_sums(forces, speeds)
    for copy in range(COLUMN):
        for c in range(3):
            for t in range(CHUNKS):
                out_ref[copy, c * 4 + t : c * 4 + t + 1, :] = forces[c][t]
        out_ref[copy, 12:16, :] = jnp.broadcast_to(sums, (4, LANES))


def column_kernel(parts_ref, vel_ref, out_ref, sums_ref):
    for z in range(COLUMN):
        for c in range(3):
            out_ref[pl.ds(c * 16 + z * 4, 4), :] = parts_ref[z, c * 4 : c * 4 + 4, :]
    out_ref[48:96, :] = vel_ref[...]
    total = sum(parts_ref[z, 12:13, :] for z in range(COLUMN))
    for n in range(sums_ref.shape[0]):
        sums_ref[n, :, :] = total


def second_kernel(
    z_ref, m_ref, o_ref, p_ref, fm_ref, fo_ref, fp_ref, sums_ref, neigh_ref, live_ref,
    out_ref, own_sums_ref, table_ref, new_ref,
):
    z = z_ref[0]
    factors = mix_factors(read_sums(jnp.sum(sums_ref[...], axis=0)))
    halo, pushed = (m_ref, o_ref, p_ref), (fm_ref, fo_ref, fp_ref)
    for a in range(3):
        for b in range(3):
            speed = new_speed(factors, pushed[a][b, 48:96, :], pushed[a][b, 0:48, :])
            new_ref[a * 3 + b, 0:48, :] = halo[a][b, 0:48, :] + time_step * speed
            new_ref[a * 3 + b, 48:64, :] = halo[a][b, 48:64, :]
            if a == 1 and b == 1:
                new_ref[9, 0:48, :] = speed
    source = lambda a, b, c, row: new_ref[a * 3 + b, pl.ds(c * 16 + row, 1), :]
    forces = own_forces(z, source, neigh_ref, live_ref, table_ref)
    own = lambda n: [
        [new_ref[n, pl.ds(c * 16 + z * 4 + t, 1), :] for t in range(CHUNKS)] for c in range(3)
    ]
    places, speeds = own(4), own(9)
    for c in range(3):
        for t in range(CHUNKS):
            out_ref[c * 4 + t : c * 4 + t + 1, :] = places[c][t]
            out_ref[12 + c * 4 + t : 13 + c * 4 + t, :] = speeds[c][t]
            out_ref[24 + c * 4 + t : 25 + c * 4 + t, :] = forces[c][t]
    sums = three_sums(forces, speeds)
    for n in range(own_sums_ref.shape[0]):
        own_sums_ref[n, :, :] = sums


def final_kernel(own_ref, sums_ref, pos_ref, vel_ref):
    factors = mix_factors(read_sums(jnp.sum(sums_ref[...], axis=0)))
    speed = new_speed(factors, own_ref[12:24, :], own_ref[24:36, :])
    place = own_ref[0:12, :] + time_step * speed
    for c in range(3):
        for t in range(CHUNKS):
            cut = pl.ds(t * LANES, LANES)
            pos_ref[c, 0, 0, :, cut] = place[c * 4 + t : c * 4 + t + 1]
            vel_ref[c, 0, 0, :, cut] = speed[c * 4 + t : c * 4 + t + 1]


def exchanged(x, axes):
    return lax.all_to_all(x, axes, 0, 0, tiled=True)


def added_for_each(parts, count):
    return jnp.broadcast_to(jnp.sum(parts, 0, keepdims=True), (count, 1, LANES))


def both_sides(x, axis):
    size = lax.axis_size(axis)
    up = [(i, (i + 1) % size) for i in range(size)]
    before = lax.ppermute(x, axis, up)
    after = lax.ppermute(x, axis, [(j, i) for i, j in up])
    return before, after


def joined(before, x, after):
    row = jnp.stack([before, x, after])
    before, after = both_sides(row, GX)
    return before, row, after


def shards(
    positions,
    velocity,
    atom_eps,
    neighbours,
    pair_live,
    event_count,
    event_atoms,
    event_weight,
    template_map,
):
    x_size, y_size = lax.axis_size(GX), lax.axis_size("gy")
    z = lax.axis_index("gz").astype(jnp.int32).reshape(1)
    inputs = (event_count, positions, velocity, atom_eps, event_weight, event_atoms)
    staged = [pltpu.VMEM(x.shape, x.dtype) for x in inputs[1:]]
    staged += [pltpu.SemaphoreType.DMA((len(staged),))]
    (own,) = call(pack_kernel, [(COLUMN, 48, LANES)], [SMEM] + [HBM] * 5, staged, None)(*inputs)
    column = exchanged(own, "gz")
    moved, speeds = call(
        events_kernel,
        [(64, LANES), (48, LANES)],
        [VMEM] * 2,
        [
            pltpu.VMEM((LIVE + EV_DEV, LANES), F32),
            pltpu.VMEM((LIVE, LANES), jnp.int32),
            pltpu.VMEM((LIVE, LANES), jnp.int32),
            pltpu.VMEM((9, LIVE, LANES), F32),
        ],
    )(column, template_map)
    before, after = both_sides(moved, "gy")
    around = joined(before, moved, after)
    table = pltpu.VMEM((4, CHUNKS, NEIGH, LANES), F32)
    (pushed,) = call(first_kernel, [(COLUMN, 16, LANES)], [SMEM] + [VMEM] * 6, [table])(
        z, *around, speeds, neighbours, pair_live
    )
    pushed = exchanged(pushed, "gz")
    forces, sums = call(column_kernel, [(96, LANES), (x_size, 1, LANES)], [VMEM] * 2)(
        pushed, speeds
    )
    before, after = both_sides(forces, "gy")
    sums = exchanged(sums, GX)
    before, after, sums = lax.optimization_barrier((before, after, sums))
    forces_around = joined(before, forces, after)
    sums = exchanged(added_for_each(sums, y_size), "gy")
    result, sums = call(
        second_kernel,
        [(40, LANES), (x_size * COLUMN, 1, LANES)],
        [SMEM] + [VMEM] * 9,
        [table, pltpu.VMEM((10, 64, LANES), F32)],
    )(z, *around, *forces_around, sums, neighbours, pair_live)
    sums = exchanged(sums, GXZ)
    sums = exchanged(added_for_each(sums, y_size), "gy")
    return tuple(
        call(final_kernel, [positions.shape, velocity.shape], [VMEM] * 2)(result, sums)
    )


def solution(mesh):
    shape = mesh.shape
    split = Mesh(
        mesh.devices.reshape(shape["gx"] // 2, 2, shape["gy"], shape["gz"]),
        ("gx_0", "gx_1", "gy", "gz"),
    )
    in_specs = (
        P(None, GX, "gy", "gz", None),
        P(None, GX, "gy", "gz", None),
        P(GX, "gy", "gz", None),
        P(GX, "gy", "gz", None, None),
        P(GX, "gy", "gz", None, None),
        P(GX, "gy", "gz"),
        P(GX, "gy", "gz", None, None),
        P(GX, "gy", "gz", None),
        P(),
    )
    out_specs = (P(None, GX, "gy", "gz", None), P(None, GX, "gy", "gz", None))
    return jax.shard_map(
        shards, mesh=split, in_specs=in_specs, out_specs=out_specs, check_vma=False
    )
```

```python
import jax
import jax.numpy as jnp
from jax import lax
from jax.experimental import pallas as pl
from jax.experimental.pallas import tpu as pltpu
from jax.sharding import Mesh
from jax.sharding import PartitionSpec as P

EV_DEV = 16
NEIGH = 32
TEMPLATE = 128
GX = ("gx_0", "gx_1")
X_Z = ("gx_0", "gz")
CORE_Y = ("gx_1", "gy")
COLUMN = 4
CHUNKS = 4
LIVE = 32
LANES = 128
F32 = jnp.float32

width_scale = 1.5
time_step = 0.1
mixing = 0.1
epsilon = 1e-06

SMEM = pl.BlockSpec(memory_space=pltpu.SMEM)
VMEM = pl.BlockSpec(memory_space=pltpu.VMEM)
HBM = pl.BlockSpec(memory_space=pltpu.HBM)


def call(kernel, outs, specs, scratch=(), limit=4 << 20, types=None):
    return pl.pallas_call(
        kernel,
        out_shape=[
            jax.ShapeDtypeStruct(shape, kind) for shape, kind in zip(outs, types or [F32] * len(outs))
        ],
        in_specs=specs,
        out_specs=[VMEM] * len(outs),
        scratch_shapes=list(scratch),
        cost_estimate=pl.CostEstimate(flops=10000, bytes_accessed=100000, transcendentals=0),
        compiler_params=pltpu.CompilerParams(vmem_limit_bytes=limit),
    )


def pack_kernel(
    count_ref, pos_hbm, vel_hbm, eps_hbm, weight_hbm, atoms_hbm, out_ref,
    pos_ref, vel_ref, eps_ref, weight_ref, atoms_ref, sems,
):
    pairs = (
        (pos_hbm, pos_ref),
        (vel_hbm, vel_ref),
        (eps_hbm, eps_ref),
        (weight_hbm, weight_ref),
        (atoms_hbm, atoms_ref),
    )
    copies = [pltpu.make_async_copy(*pair, sems.at[n]) for n, pair in enumerate(pairs)]
    for copy in copies:
        copy.start()
    for copy in range(COLUMN):
        out_ref[copy, 24:32, :] = jnp.zeros((8, LANES), F32)
    for copy in copies:
        copy.wait()
    count = count_ref[0, 0, 0]
    live = lax.broadcasted_iota(jnp.int32, (1, EV_DEV), 1) < count
    weights = jnp.where(live, weight_ref[0, 0, :, :], 0.0)
    counts = jnp.full((1, LANES), count, jnp.int32).astype(F32)
    atoms = atoms_ref[0, 0, 0, :, :].astype(F32)
    for copy in range(COLUMN):
        for c in range(3):
            for q in range(CHUNKS):
                cut = pl.ds(q * LANES, LANES)
                out_ref[copy, c * 4 + q : c * 4 + q + 1, :] = pos_ref[c, 0, 0, :, cut]
                out_ref[copy, 16 + c * 4 + q : 17 + c * 4 + q, :] = vel_ref[c, 0, 0, :, cut]
        for q in range(CHUNKS):
            out_ref[copy, 12 + q : 13 + q, :] = eps_ref[0, 0, :, pl.ds(q * LANES, LANES)]
        out_ref[copy, 28:29, 0:EV_DEV] = weights
        out_ref[copy, 29:30, :] = counts
        out_ref[copy, 32:48, :] = atoms


def events_kernel(
    column_ref, map_ref, neigh_ref, live_ref, moved_ref, vel_ref, pairs_ref,
    atoms_ref, low_ref, high_ref, shift_ref,
):
    pairs_ref[0:NEIGH, :] = neigh_ref[0, 0, 0, :, :]
    pairs_ref[NEIGH:, :] = live_ref[0, 0, 0, :, :]
    atoms_ref[...] = jnp.zeros(atoms_ref.shape, F32)
    first = jnp.int32(0)
    lane_weights = jnp.zeros((1, LANES), F32)
    for z in range(COLUMN):
        for e in range(EV_DEV):
            atoms_ref[pl.ds(first + e, 1), :] = column_ref[z, 32 + e : 33 + e, :]
        lane_weights = lane_weights + pltpu.roll(column_ref[z, 28:29, :], first, 1)
        if z < COLUMN - 1:
            first = first + jnp.max(column_ref[z, 29:30, :]).astype(jnp.int32)
    atoms = atoms_ref[0:LIVE, :].astype(jnp.int32)
    low, high = atoms & (LANES - 1), atoms >> 7
    low_ref[...] = low
    high_ref[...] = high
    slot = lax.broadcasted_iota(jnp.int32, (LIVE, LANES), 0)
    lane = lax.broadcasted_iota(jnp.int32, (LIVE, LANES), 1)
    weights = jnp.sum(jnp.where(slot == lane, lane_weights, 0.0), axis=1, keepdims=True)
    centred = []
    for c in range(3):
        taken = jnp.zeros((LIVE, LANES), F32)
        for h in range(COLUMN * CHUNKS):
            z, q = divmod(h, CHUNKS)
            row = jnp.broadcast_to(column_ref[z, c * 4 + q : c * 4 + q + 1, :], (LIVE, LANES))
            taken = jnp.where(high == h, jnp.take_along_axis(row, low, axis=1), taken)
        centred.append(taken - jnp.sum(taken, axis=1, keepdims=True) * (1.0 / TEMPLATE))
    shift = jnp.dot(
        jnp.concatenate(centred, 0),
        map_ref[...],
        precision=lax.Precision.HIGHEST,
        preferred_element_type=F32,
    )
    shift = shift * jnp.concatenate([weights] * 3, 0)
    for part in range(3):
        rounded = shift.astype(jnp.bfloat16).astype(F32)
        for c in range(3):
            shift_ref[part * 3 + c, :, :] = rounded[c * LIVE : (c + 1) * LIVE]
        shift = shift - rounded
    places = lax.broadcasted_iota(jnp.int32, (LANES, LANES), 0)
    rows = lax.broadcasted_iota(jnp.int32, (16, LANES), 0)
    total = jnp.zeros((144, LANES), F32)
    for i in range(LIVE // 4):
        lefts, rights = [], []
        for j in range(4):
            e = slice(i * 4 + j, i * 4 + j + 1)
            here = high_ref[e, :] == rows
            left = [jnp.where(here, shift_ref[n, e, :], 0.0) for n in range(9)]
            lefts.append(jnp.concatenate(left, 0).astype(jnp.bfloat16))
            rights.append(jnp.where(low_ref[e, :] == places, 1.0, 0.0).astype(jnp.bfloat16))
        total = total + lax.dot_general(
            jnp.concatenate(lefts, 1),
            jnp.concatenate(rights, 1),
            (((1,), (1,)), ((), ())),
            preferred_element_type=F32,
        )
    displaced = total[0:48] + total[48:96] + total[96:144]
    for z in range(COLUMN):
        for c in range(3):
            there = pl.ds(c * 16 + z * 4, 4)
            moved_ref[there, :] = (
                column_ref[z, c * 4 : c * 4 + 4, :] + displaced[c * 16 + z * 4 : c * 16 + z * 4 + 4]
            )
            vel_ref[there, :] = column_ref[z, 16 + c * 4 : 20 + c * 4, :]
        moved_ref[pl.ds(48 + z * 4, 4), :] = column_ref[z, 12:16, :]


def domain_forces(z, firsts, source, pairs_ref, table_ref):
    for a in range(3):
        for b in range(3):
            for dz in range(3):
                k = firsts[a][b] + dz
                first = ((z + dz + 3) & 3) * 4
                for c in range(4):
                    for q in range(CHUNKS):
                        table_ref[c, q, pl.ds(k, 1), :] = source(a, b, c, first + q)
    for c in range(4):
        for q in range(CHUNKS):
            table_ref[c, q, 27:NEIGH, :] = table_ref[c, q, 0 : NEIGH - 27, :]
    forces = [[None] * CHUNKS for _ in range(3)]
    for t in range(CHUNKS):
        own = [source(1, 1, c, z * 4 + t) for c in range(4)]
        total = [jnp.zeros((8, LANES), F32)] * 3
        cut = pl.ds(t * LANES, LANES)
        for g in range(NEIGH // 8):
            atoms = pairs_ref[8 * g : 8 * g + 8, cut]
            live = pairs_ref[NEIGH + 8 * g : NEIGH + 8 * g + 8, cut].astype(F32)
            low, high = atoms & (LANES - 1), atoms >> 7
            taken = []
            for c in range(4):
                value = jnp.take_along_axis(table_ref[c, 0, 8 * g : 8 * g + 8, :], low, axis=1)
                for q in range(1, CHUNKS):
                    other = jnp.take_along_axis(table_ref[c, q, 8 * g : 8 * g + 8, :], low, axis=1)
                    value = jnp.where(high == q, other, value)
                taken.append(value)
            apart = [own[c] - taken[c] for c in range(3)]
            square = apart[0] * apart[0] + apart[1] * apart[1] + apart[2] * apart[2]
            strength = jnp.sqrt(own[3] * taken[3]) * live
            strength = (
                strength
                * jnp.exp(-square * (0.5 / (width_scale * width_scale)))
                * (1.0 / (width_scale * width_scale))
            )
            total = [total[c] + strength * apart[c] for c in range(3)]
        for c in range(3):
            forces[c][t] = jnp.sum(total[c], axis=0, keepdims=True)
    return forces


def directions(where_ref):
    odd = [where_ref[n] & 1 for n in range(2)]
    spots = [(2 - 2 * flag, 1, 2 * flag) for flag in odd]
    return [[9 * a + 3 * b for b in spots[1]] for a in spots[0]]


def three_sums(forces, speeds):
    pairs = ((forces, speeds), (speeds, speeds), (forces, forces))
    lane = lax.broadcasted_iota(jnp.int32, (1, LANES), 1)
    packed = jnp.zeros((1, LANES), F32)
    for n, (left, right) in enumerate(pairs):
        added = sum(left[c][t] * right[c][t] for c in range(3) for t in range(CHUNKS))
        packed = jnp.where(lane == n, jnp.sum(added, axis=1, keepdims=True), packed)
    return packed


def read_sums(summed):
    lane = lax.broadcasted_iota(jnp.int32, (1, LANES), 1)
    return [
        jnp.sum(jnp.where(lane == n, summed, 0.0), axis=1, keepdims=True) for n in range(3)
    ]


def mix_factors(sums):
    power_sum, speed_sq, force_sq = sums
    cosine = power_sum / (jnp.sqrt(speed_sq + epsilon) * jnp.sqrt(force_sq + epsilon))
    speed_ratio = jnp.sqrt((speed_sq + epsilon) / (force_sq + epsilon))
    return 0.5 * (1.0 + cosine), mixing * speed_ratio


def new_speed(factors, speed, force):
    scale, ratio = factors
    return scale * ((1.0 - mixing) * speed + ratio * force) + time_step * force


def first_kernel(
    where_ref, m_ref, o_ref, p_ref, vel_ref, pairs_ref, pairs_m_ref, pairs_p_ref,
    out_ref, sums_ref, table_ref,
):
    z = where_ref[2]
    step = 1 - 2 * (z & 1)
    firsts = directions(where_ref)
    halo = (m_ref, o_ref, p_ref)
    source = lambda a, b, c, row: halo[a][b, pl.ds(c * 16 + row, 1), :]
    out_ref[0:48, :] = jnp.zeros((48, LANES), F32)
    out_ref[48:96, :] = vel_ref[...]
    places = ((z, pairs_ref), ((z + step) & 3, pairs_m_ref), ((z - step) & 3, pairs_p_ref))
    for place, pairs in places:
        forces = domain_forces(place, firsts, source, pairs, table_ref)
        for c in range(3):
            for t in range(CHUNKS):
                out_ref[pl.ds(c * 16 + place * 4 + t, 1), :] = forces[c][t]
        if pairs is pairs_ref:
            speeds = [
                [vel_ref[pl.ds(c * 16 + z * 4 + t, 1), :] for t in range(CHUNKS)]
                for c in range(3)
            ]
            sums = three_sums(forces, speeds)
            for n in range(sums_ref.shape[0]):
                sums_ref[n, :, :] = sums


def second_kernel(
    where_ref, m_ref, o_ref, p_ref, fm_ref, fo_ref, fp_ref, sums_ref, pairs_ref,
    out_ref, own_sums_ref, table_ref, new_ref,
):
    z = where_ref[2]
    factors = mix_factors(read_sums(jnp.sum(sums_ref[...], axis=0)))
    halo, pushed = (m_ref, o_ref, p_ref), (fm_ref, fo_ref, fp_ref)
    for a in range(3):
        for b in range(3):
            speed = new_speed(factors, pushed[a][b, 48:96, :], pushed[a][b, 0:48, :])
            new_ref[a * 3 + b, 0:48, :] = halo[a][b, 0:48, :] + time_step * speed
            new_ref[a * 3 + b, 48:64, :] = halo[a][b, 48:64, :]
            if a == 1 and b == 1:
                new_ref[9, 0:48, :] = speed
    source = lambda a, b, c, row: new_ref[a * 3 + b, pl.ds(c * 16 + row, 1), :]
    forces = domain_forces(z, directions(where_ref), source, pairs_ref, table_ref)
    own = lambda n: [
        [new_ref[n, pl.ds(c * 16 + z * 4 + t, 1), :] for t in range(CHUNKS)] for c in range(3)
    ]
    places, speeds = own(4), own(9)
    for c in range(3):
        for t in range(CHUNKS):
            out_ref[c * 4 + t : c * 4 + t + 1, :] = places[c][t]
            out_ref[12 + c * 4 + t : 13 + c * 4 + t, :] = speeds[c][t]
            out_ref[24 + c * 4 + t : 25 + c * 4 + t, :] = forces[c][t]
    sums = three_sums(forces, speeds)
    for n in range(own_sums_ref.shape[0]):
        own_sums_ref[n, :, :] = sums


def final_kernel(own_ref, sums_ref, pos_ref, vel_ref):
    factors = mix_factors(read_sums(jnp.sum(sums_ref[...], axis=0)))
    speed = new_speed(factors, own_ref[12:24, :], own_ref[24:36, :])
    place = own_ref[0:12, :] + time_step * speed
    for c in range(3):
        for t in range(CHUNKS):
            cut = pl.ds(t * LANES, LANES)
            pos_ref[c, 0, 0, :, cut] = place[c * 4 + t : c * 4 + t + 1]
            vel_ref[c, 0, 0, :, cut] = speed[c * 4 + t : c * 4 + t + 1]


def exchanged(x, axes):
    return lax.all_to_all(x, axes, 0, 0, tiled=True)


def added_for_each(parts, count):
    return jnp.broadcast_to(jnp.sum(parts, 0, keepdims=True), (count, 1, LANES))


def both_sides(x, axis):
    size = lax.axis_size(axis)
    first = [(i, i ^ 1) for i in range(size)]
    second = [(i, (i - 1 + 2 * (i % 2)) % size) for i in range(size)]
    return lax.ppermute(x, axis, first), lax.ppermute(x, axis, second)


def halves(x):
    first, second = both_sides(x, "gy")
    return first, x, second


def joined(first, x, second):
    row = jnp.stack([first, x, second])
    first, second = both_sides(row, GX)
    return first, row, second


def shards(
    positions,
    velocity,
    atom_eps,
    neighbours,
    pair_live,
    event_count,
    event_atoms,
    event_weight,
    template_map,
):
    half_x, size_y = lax.axis_size("gx_0"), lax.axis_size("gy")
    where = jnp.stack([lax.axis_index(axis) for axis in ("gx_1", "gy", "gz")]).astype(jnp.int32)
    inputs = (event_count, positions, velocity, atom_eps, event_weight, event_atoms)
    staged = [pltpu.VMEM(x.shape, x.dtype) for x in inputs[1:]]
    staged += [pltpu.SemaphoreType.DMA((len(staged),))]
    (own,) = call(pack_kernel, [(COLUMN, 48, LANES)], [SMEM] + [HBM] * 5, staged, None)(*inputs)
    column = exchanged(own, "gz")
    moved, speeds, pairs = call(
        events_kernel,
        [(64, LANES), (48, LANES), (2 * NEIGH, CHUNKS * LANES)],
        [VMEM] * 4,
        [
            pltpu.VMEM((LIVE + EV_DEV, LANES), F32),
            pltpu.VMEM((LIVE, LANES), jnp.int32),
            pltpu.VMEM((LIVE, LANES), jnp.int32),
            pltpu.VMEM((9, LIVE, LANES), F32),
        ],
        types=[F32, F32, jnp.int32],
    )(column, template_map, neighbours, pair_live)
    around = joined(*halves(moved))
    table = pltpu.VMEM((4, CHUNKS, NEIGH, LANES), F32)
    forces, sums = call(
        first_kernel, [(96, LANES), (half_x * COLUMN, 1, LANES)], [SMEM] + [VMEM] * 7, [table]
    )(where, *around, speeds, pairs, *both_sides(pairs, "gz"))
    first, forces, second = halves(forces)
    sums = exchanged(sums, X_Z)
    first, second, sums = lax.optimization_barrier((first, second, sums))
    forces_around = joined(first, forces, second)
    sums = exchanged(added_for_each(sums, 2 * size_y), CORE_Y)
    result, sums = call(
        second_kernel,
        [(40, LANES), (half_x * COLUMN, 1, LANES)],
        [SMEM] + [VMEM] * 8,
        [table, pltpu.VMEM((10, 64, LANES), F32)],
    )(where, *around, *forces_around, sums, pairs)
    sums = exchanged(sums, X_Z)
    sums = exchanged(added_for_each(sums, 2 * size_y), CORE_Y)
    return tuple(
        call(final_kernel, [positions.shape, velocity.shape], [VMEM] * 2)(result, sums)
    )


def solution(mesh):
    shape = mesh.shape
    split = Mesh(
        mesh.devices.reshape(shape["gx"] // 2, 2, shape["gy"], shape["gz"]),
        ("gx_0", "gx_1", "gy", "gz"),
    )
    in_specs = (
        P(None, GX, "gy", "gz", None),
        P(None, GX, "gy", "gz", None),
        P(GX, "gy", "gz", None),
        P(GX, "gy", "gz", None, None),
        P(GX, "gy", "gz", None, None),
        P(GX, "gy", "gz"),
        P(GX, "gy", "gz", None, None),
        P(GX, "gy", "gz", None),
        P(),
    )
    out_specs = (P(None, GX, "gy", "gz", None), P(None, GX, "gy", "gz", None))
    return jax.shard_map(
        shards, mesh=split, in_specs=in_specs, out_specs=out_specs, check_vma=False
    )
```

```python
import jax
import jax.numpy as jnp
from jax import lax
from jax.experimental import pallas as pl
from jax.experimental.pallas import tpu as pltpu
from jax.sharding import Mesh
from jax.sharding import PartitionSpec as P


EV_DEV = 16
NEIGH = 32
TEMPLATE = 128
GX = ("gx_0", "gx_1")
GXZ = ("gx_0", "gx_1", "gz")
COLUMN = 4
CHUNKS = 4
LIVE = 32
LANES = 128
F32 = jnp.float32

width_scale = 1.5
time_step = 0.1
mixing = 0.1
epsilon = 1e-06

SMEM = pl.BlockSpec(memory_space=pltpu.SMEM)
VMEM = pl.BlockSpec(memory_space=pltpu.VMEM)
HBM = pl.BlockSpec(memory_space=pltpu.HBM)


def call(kernel, outs, specs, scratch=(), limit=4 << 20):
    return pl.pallas_call(
        kernel,
        out_shape=[jax.ShapeDtypeStruct(shape, F32) for shape in outs],
        in_specs=specs,
        out_specs=[VMEM] * len(outs),
        scratch_shapes=list(scratch),
        cost_estimate=pl.CostEstimate(flops=10000, bytes_accessed=100000, transcendentals=0),
        compiler_params=pltpu.CompilerParams(vmem_limit_bytes=limit),
    )


def pack_kernel(
    count_ref, pos_hbm, vel_hbm, eps_hbm, weight_hbm, atoms_hbm, out_ref,
    pos_ref, vel_ref, eps_ref, weight_ref, atoms_ref, sems,
):
    pairs = (
        (pos_hbm, pos_ref),
        (vel_hbm, vel_ref),
        (eps_hbm, eps_ref),
        (weight_hbm, weight_ref),
        (atoms_hbm, atoms_ref),
    )
    copies = [pltpu.make_async_copy(*pair, sems.at[n]) for n, pair in enumerate(pairs)]
    for copy in copies:
        copy.start()
    for copy in range(COLUMN):
        out_ref[copy, 24:32, :] = jnp.zeros((8, LANES), F32)
    for copy in copies:
        copy.wait()
    count = count_ref[0, 0, 0]
    live = lax.broadcasted_iota(jnp.int32, (1, EV_DEV), 1) < count
    weights = jnp.where(live, weight_ref[0, 0, :, :], 0.0)
    counts = jnp.full((1, LANES), count, jnp.int32).astype(F32)
    atoms = atoms_ref[0, 0, 0, :, :].astype(F32)
    for copy in range(COLUMN):
        for c in range(3):
            for q in range(CHUNKS):
                cut = pl.ds(q * LANES, LANES)
                out_ref[copy, c * 4 + q : c * 4 + q + 1, :] = pos_ref[c, 0, 0, :, cut]
                out_ref[copy, 16 + c * 4 + q : 17 + c * 4 + q, :] = vel_ref[c, 0, 0, :, cut]
        for q in range(CHUNKS):
            out_ref[copy, 12 + q : 13 + q, :] = eps_ref[0, 0, :, pl.ds(q * LANES, LANES)]
        out_ref[copy, 28:29, 0:EV_DEV] = weights
        out_ref[copy, 29:30, :] = counts
        out_ref[copy, 32:48, :] = atoms


def events_kernel(column_ref, map_ref, moved_ref, vel_ref, atoms_ref, low_ref, high_ref, shift_ref):
    atoms_ref[...] = jnp.zeros(atoms_ref.shape, F32)
    first = jnp.int32(0)
    lane_weights = jnp.zeros((1, LANES), F32)
    for z in range(COLUMN):
        for e in range(EV_DEV):
            atoms_ref[pl.ds(first + e, 1), :] = column_ref[z, 32 + e : 33 + e, :]
        lane_weights = lane_weights + pltpu.roll(column_ref[z, 28:29, :], first, 1)
        if z < COLUMN - 1:
            first = first + jnp.max(column_ref[z, 29:30, :]).astype(jnp.int32)
    atoms = atoms_ref[0:LIVE, :].astype(jnp.int32)
    low, high = atoms & (LANES - 1), atoms >> 7
    low_ref[...] = low
    high_ref[...] = high
    slot = lax.broadcasted_iota(jnp.int32, (LIVE, LANES), 0)
    lane = lax.broadcasted_iota(jnp.int32, (LIVE, LANES), 1)
    weights = jnp.sum(jnp.where(slot == lane, lane_weights, 0.0), axis=1, keepdims=True)
    centred = []
    for c in range(3):
        taken = jnp.zeros((LIVE, LANES), F32)
        for h in range(COLUMN * CHUNKS):
            z, q = divmod(h, CHUNKS)
            row = jnp.broadcast_to(column_ref[z, c * 4 + q : c * 4 + q + 1, :], (LIVE, LANES))
            taken = jnp.where(high == h, jnp.take_along_axis(row, low, axis=1), taken)
        centred.append(taken - jnp.sum(taken, axis=1, keepdims=True) * (1.0 / TEMPLATE))
    shift = jnp.dot(
        jnp.concatenate(centred, 0),
        map_ref[...],
        precision=lax.Precision.HIGHEST,
        preferred_element_type=F32,
    )
    shift = shift * jnp.concatenate([weights] * 3, 0)
    for part in range(3):
        rounded = shift.astype(jnp.bfloat16).astype(F32)
        for c in range(3):
            shift_ref[part * 3 + c, :, :] = rounded[c * LIVE : (c + 1) * LIVE]
        shift = shift - rounded
    places = lax.broadcasted_iota(jnp.int32, (LANES, LANES), 0)
    rows = lax.broadcasted_iota(jnp.int32, (16, LANES), 0)
    total = jnp.zeros((144, LANES), F32)
    for i in range(LIVE // 4):
        lefts, rights = [], []
        for j in range(4):
            e = slice(i * 4 + j, i * 4 + j + 1)
            here = high_ref[e, :] == rows
            left = [jnp.where(here, shift_ref[n, e, :], 0.0) for n in range(9)]
            lefts.append(jnp.concatenate(left, 0).astype(jnp.bfloat16))
            rights.append(jnp.where(low_ref[e, :] == places, 1.0, 0.0).astype(jnp.bfloat16))
        total = total + lax.dot_general(
            jnp.concatenate(lefts, 1),
            jnp.concatenate(rights, 1),
            (((1,), (1,)), ((), ())),
            preferred_element_type=F32,
        )
    displaced = total[0:48] + total[48:96] + total[96:144]
    for z in range(COLUMN):
        for c in range(3):
            there = pl.ds(c * 16 + z * 4, 4)
            moved_ref[there, :] = (
                column_ref[z, c * 4 : c * 4 + 4, :] + displaced[c * 16 + z * 4 : c * 16 + z * 4 + 4]
            )
            vel_ref[there, :] = column_ref[z, 16 + c * 4 : 20 + c * 4, :]
        moved_ref[pl.ds(48 + z * 4, 4), :] = column_ref[z, 12:16, :]


def own_forces(z, source, neigh_ref, live_ref, table_ref):
    for k in range(NEIGH):
        ab, dz = divmod(k % 27, 3)
        a, b = divmod(ab, 3)
        first = ((z + dz + 3) & 3) * 4
        for c in range(4):
            for q in range(CHUNKS):
                table_ref[c, q, k : k + 1, :] = source(a, b, c, first + q)
    forces = [[None] * CHUNKS for _ in range(3)]
    for t in range(CHUNKS):
        own = [source(1, 1, c, z * 4 + t) for c in range(4)]
        total = [jnp.zeros((8, LANES), F32)] * 3
        for g in range(NEIGH // 8):
            atoms = neigh_ref[0, 0, 0, 8 * g : 8 * g + 8, t * LANES : (t + 1) * LANES]
            live = live_ref[0, 0, 0, 8 * g : 8 * g + 8, t * LANES : (t + 1) * LANES].astype(F32)
            low, high = atoms & (LANES - 1), atoms >> 7
            taken = []
            for c in range(4):
                value = jnp.take_along_axis(table_ref[c, 0, 8 * g : 8 * g + 8, :], low, axis=1)
                for q in range(1, CHUNKS):
                    other = jnp.take_along_axis(table_ref[c, q, 8 * g : 8 * g + 8, :], low, axis=1)
                    value = jnp.where(high == q, other, value)
                taken.append(value)
            apart = [own[c] - taken[c] for c in range(3)]
            square = apart[0] * apart[0] + apart[1] * apart[1] + apart[2] * apart[2]
            strength = jnp.sqrt(own[3] * taken[3]) * live
            strength = (
                strength
                * jnp.exp(-square * (0.5 / (width_scale * width_scale)))
                * (1.0 / (width_scale * width_scale))
            )
            total = [total[c] + strength * apart[c] for c in range(3)]
        for c in range(3):
            forces[c][t] = jnp.sum(total[c], axis=0, keepdims=True)
    return forces


def three_sums(forces, speeds):
    pairs = ((forces, speeds), (speeds, speeds), (forces, forces))
    lane = lax.broadcasted_iota(jnp.int32, (1, LANES), 1)
    packed = jnp.zeros((1, LANES), F32)
    for n, (left, right) in enumerate(pairs):
        added = sum(left[c][t] * right[c][t] for c in range(3) for t in range(CHUNKS))
        packed = jnp.where(lane == n, jnp.sum(added, axis=1, keepdims=True), packed)
    return packed


def read_sums(summed):
    lane = lax.broadcasted_iota(jnp.int32, (1, LANES), 1)
    return [
        jnp.sum(jnp.where(lane == n, summed, 0.0), axis=1, keepdims=True) for n in range(3)
    ]


def mix_factors(sums):
    power_sum, speed_sq, force_sq = sums
    cosine = power_sum / (jnp.sqrt(speed_sq + epsilon) * jnp.sqrt(force_sq + epsilon))
    speed_ratio = jnp.sqrt((speed_sq + epsilon) / (force_sq + epsilon))
    return 0.5 * (1.0 + cosine), mixing * speed_ratio


def new_speed(factors, speed, force):
    scale, ratio = factors
    return scale * ((1.0 - mixing) * speed + ratio * force) + time_step * force


def first_kernel(z_ref, m_ref, o_ref, p_ref, vel_ref, neigh_ref, live_ref, out_ref, table_ref):
    z = z_ref[0]
    halo = (m_ref, o_ref, p_ref)
    source = lambda a, b, c, row: halo[a][b, pl.ds(c * 16 + row, 1), :]
    forces = own_forces(z, source, neigh_ref, live_ref, table_ref)
    speeds = [
        [vel_ref[pl.ds(c * 16 + z * 4 + t, 1), :] for t in range(CHUNKS)] for c in range(3)
    ]
    sums = three_sums(forces, speeds)
    for copy in range(COLUMN):
        for c in range(3):
            for t in range(CHUNKS):
                out_ref[copy, c * 4 + t : c * 4 + t + 1, :] = forces[c][t]
        out_ref[copy, 12:16, :] = jnp.broadcast_to(sums, (4, LANES))


def column_kernel(parts_ref, vel_ref, out_ref, sums_ref):
    for z in range(COLUMN):
        for c in range(3):
            out_ref[pl.ds(c * 16 + z * 4, 4), :] = parts_ref[z, c * 4 : c * 4 + 4, :]
    out_ref[48:96, :] = vel_ref[...]
    total = sum(parts_ref[z, 12:13, :] for z in range(COLUMN))
    for n in range(sums_ref.shape[0]):
        sums_ref[n, :, :] = total


def second_kernel(
    z_ref, m_ref, o_ref, p_ref, fm_ref, fo_ref, fp_ref, sums_ref, neigh_ref, live_ref,
    out_ref, own_sums_ref, table_ref, new_ref,
):
    z = z_ref[0]
    factors = mix_factors(read_sums(jnp.sum(sums_ref[...], axis=0)))
    halo, pushed = (m_ref, o_ref, p_ref), (fm_ref, fo_ref, fp_ref)
    for a in range(3):
        for b in range(3):
            speed = new_speed(factors, pushed[a][b, 48:96, :], pushed[a][b, 0:48, :])
            new_ref[a * 3 + b, 0:48, :] = halo[a][b, 0:48, :] + time_step * speed
            new_ref[a * 3 + b, 48:64, :] = halo[a][b, 48:64, :]
            if a == 1 and b == 1:
                new_ref[9, 0:48, :] = speed
    source = lambda a, b, c, row: new_ref[a * 3 + b, pl.ds(c * 16 + row, 1), :]
    forces = own_forces(z, source, neigh_ref, live_ref, table_ref)
    own = lambda n: [
        [new_ref[n, pl.ds(c * 16 + z * 4 + t, 1), :] for t in range(CHUNKS)] for c in range(3)
    ]
    places, speeds = own(4), own(9)
    for c in range(3):
        for t in range(CHUNKS):
            out_ref[c * 4 + t : c * 4 + t + 1, :] = places[c][t]
            out_ref[12 + c * 4 + t : 13 + c * 4 + t, :] = speeds[c][t]
            out_ref[24 + c * 4 + t : 25 + c * 4 + t, :] = forces[c][t]
    sums = three_sums(forces, speeds)
    for n in range(own_sums_ref.shape[0]):
        own_sums_ref[n, :, :] = sums


def final_kernel(own_ref, sums_ref, pos_ref, vel_ref):
    factors = mix_factors(read_sums(jnp.sum(sums_ref[...], axis=0)))
    speed = new_speed(factors, own_ref[12:24, :], own_ref[24:36, :])
    place = own_ref[0:12, :] + time_step * speed
    for c in range(3):
        for t in range(CHUNKS):
            cut = pl.ds(t * LANES, LANES)
            pos_ref[c, 0, 0, :, cut] = place[c * 4 + t : c * 4 + t + 1]
            vel_ref[c, 0, 0, :, cut] = speed[c * 4 + t : c * 4 + t + 1]


def exchanged(x, axes):
    return lax.all_to_all(x, axes, 0, 0, tiled=True)


def added_for_each(parts, count):
    return jnp.broadcast_to(jnp.sum(parts, 0, keepdims=True), (count, 1, LANES))


def both_sides(x, axis):
    size = lax.axis_size(axis)
    up = [(i, (i + 1) % size) for i in range(size)]
    before = lax.ppermute(x, axis, up)
    after = lax.ppermute(x, axis, [(j, i) for i, j in up])
    return before, after


def joined(before, x, after):
    row = jnp.stack([before, x, after])
    before, after = both_sides(row, GX)
    return before, row, after


def shards(
    positions,
    velocity,
    atom_eps,
    neighbours,
    pair_live,
    event_count,
    event_atoms,
    event_weight,
    template_map,
):
    x_size, y_size = lax.axis_size(GX), lax.axis_size("gy")
    z = lax.axis_index("gz").astype(jnp.int32).reshape(1)
    inputs = (event_count, positions, velocity, atom_eps, event_weight, event_atoms)
    staged = [pltpu.VMEM(x.shape, x.dtype) for x in inputs[1:]]
    staged += [pltpu.SemaphoreType.DMA((len(staged),))]
    (own,) = call(pack_kernel, [(COLUMN, 48, LANES)], [SMEM] + [HBM] * 5, staged, None)(*inputs)
    column = exchanged(own, "gz")
    moved, speeds = call(
        events_kernel,
        [(64, LANES), (48, LANES)],
        [VMEM] * 2,
        [
            pltpu.VMEM((LIVE + EV_DEV, LANES), F32),
            pltpu.VMEM((LIVE, LANES), jnp.int32),
            pltpu.VMEM((LIVE, LANES), jnp.int32),
            pltpu.VMEM((9, LIVE, LANES), F32),
        ],
    )(column, template_map)
    before, after = both_sides(moved, "gy")
    around = joined(before, moved, after)
    table = pltpu.VMEM((4, CHUNKS, NEIGH, LANES), F32)
    (pushed,) = call(first_kernel, [(COLUMN, 16, LANES)], [SMEM] + [VMEM] * 6, [table])(
        z, *around, speeds, neighbours, pair_live
    )
    pushed = exchanged(pushed, "gz")
    forces, sums = call(column_kernel, [(96, LANES), (y_size, 1, LANES)], [VMEM] * 2)(
        pushed, speeds
    )
    sums = exchanged(sums, "gy")
    before, after = both_sides(forces, "gy")
    before, after, sums = lax.optimization_barrier((before, after, sums))
    forces_around = joined(before, forces, after)
    sums = exchanged(added_for_each(sums, x_size), GX)
    result, sums = call(
        second_kernel,
        [(40, LANES), (x_size * COLUMN, 1, LANES)],
        [SMEM] + [VMEM] * 9,
        [table, pltpu.VMEM((10, 64, LANES), F32)],
    )(z, *around, *forces_around, sums, neighbours, pair_live)
    sums = exchanged(sums, GXZ)
    sums = exchanged(added_for_each(sums, y_size), "gy")
    return tuple(
        call(final_kernel, [positions.shape, velocity.shape], [VMEM] * 2)(result, sums)
    )


def solution(mesh):
    shape = mesh.shape
    split = Mesh(
        mesh.devices.reshape(shape["gx"] // 2, 2, shape["gy"], shape["gz"]),
        ("gx_0", "gx_1", "gy", "gz"),
    )
    in_specs = (
        P(None, GX, "gy", "gz", None),
        P(None, GX, "gy", "gz", None),
        P(GX, "gy", "gz", None),
        P(GX, "gy", "gz", None, None),
        P(GX, "gy", "gz", None, None),
        P(GX, "gy", "gz"),
        P(GX, "gy", "gz", None, None),
        P(GX, "gy", "gz", None),
        P(),
    )
    out_specs = (P(None, GX, "gy", "gz", None), P(None, GX, "gy", "gz", None))
    return jax.shard_map(
        shards, mesh=split, in_specs=in_specs, out_specs=out_specs, check_vma=False
    )
```

```python
import jax
import jax.numpy as jnp
from jax import lax
from jax.experimental import pallas as pl
from jax.experimental.pallas import tpu as pltpu
from jax.sharding import Mesh
from jax.sharding import PartitionSpec as P


EV_DEV = 16
NEIGH = 32
TEMPLATE = 128
GX = ("gx_0", "gx_1")
GXZ = ("gx_0", "gx_1", "gz")
X_Y = ("gx_0", "gy")
CORE_Z = ("gx_1", "gz")
COLUMN = 4
CHUNKS = 4
LIVE = 32
LANES = 128
F32 = jnp.float32

width_scale = 1.5
time_step = 0.1
mixing = 0.1
epsilon = 1e-06

SMEM = pl.BlockSpec(memory_space=pltpu.SMEM)
VMEM = pl.BlockSpec(memory_space=pltpu.VMEM)
HBM = pl.BlockSpec(memory_space=pltpu.HBM)


def call(kernel, outs, specs, scratch=(), limit=4 << 20):
    return pl.pallas_call(
        kernel,
        out_shape=[jax.ShapeDtypeStruct(shape, F32) for shape in outs],
        in_specs=specs,
        out_specs=[VMEM] * len(outs),
        scratch_shapes=list(scratch),
        cost_estimate=pl.CostEstimate(flops=10000, bytes_accessed=100000, transcendentals=0),
        compiler_params=pltpu.CompilerParams(vmem_limit_bytes=limit),
    )


def pack_kernel(
    count_ref, pos_hbm, vel_hbm, eps_hbm, weight_hbm, atoms_hbm, out_ref,
    pos_ref, vel_ref, eps_ref, weight_ref, atoms_ref, sems,
):
    pairs = (
        (pos_hbm, pos_ref),
        (vel_hbm, vel_ref),
        (eps_hbm, eps_ref),
        (weight_hbm, weight_ref),
        (atoms_hbm, atoms_ref),
    )
    copies = [pltpu.make_async_copy(*pair, sems.at[n]) for n, pair in enumerate(pairs)]
    for copy in copies:
        copy.start()
    for copy in range(COLUMN):
        out_ref[copy, 24:32, :] = jnp.zeros((8, LANES), F32)
    for copy in copies:
        copy.wait()
    count = count_ref[0, 0, 0]
    live = lax.broadcasted_iota(jnp.int32, (1, EV_DEV), 1) < count
    weights = jnp.where(live, weight_ref[0, 0, :, :], 0.0)
    counts = jnp.full((1, LANES), count, jnp.int32).astype(F32)
    atoms = atoms_ref[0, 0, 0, :, :].astype(F32)
    for copy in range(COLUMN):
        for c in range(3):
            for q in range(CHUNKS):
                cut = pl.ds(q * LANES, LANES)
                out_ref[copy, c * 4 + q : c * 4 + q + 1, :] = pos_ref[c, 0, 0, :, cut]
                out_ref[copy, 16 + c * 4 + q : 17 + c * 4 + q, :] = vel_ref[c, 0, 0, :, cut]
        for q in range(CHUNKS):
            out_ref[copy, 12 + q : 13 + q, :] = eps_ref[0, 0, :, pl.ds(q * LANES, LANES)]
        out_ref[copy, 28:29, 0:EV_DEV] = weights
        out_ref[copy, 29:30, :] = counts
        out_ref[copy, 32:48, :] = atoms


def events_kernel(column_ref, map_ref, moved_ref, vel_ref, atoms_ref, low_ref, high_ref, shift_ref):
    atoms_ref[...] = jnp.zeros(atoms_ref.shape, F32)
    first = jnp.int32(0)
    lane_weights = jnp.zeros((1, LANES), F32)
    for z in range(COLUMN):
        for e in range(EV_DEV):
            atoms_ref[pl.ds(first + e, 1), :] = column_ref[z, 32 + e : 33 + e, :]
        lane_weights = lane_weights + pltpu.roll(column_ref[z, 28:29, :], first, 1)
        if z < COLUMN - 1:
            first = first + jnp.max(column_ref[z, 29:30, :]).astype(jnp.int32)
    atoms = atoms_ref[0:LIVE, :].astype(jnp.int32)
    low, high = atoms & (LANES - 1), atoms >> 7
    low_ref[...] = low
    high_ref[...] = high
    slot = lax.broadcasted_iota(jnp.int32, (LIVE, LANES), 0)
    lane = lax.broadcasted_iota(jnp.int32, (LIVE, LANES), 1)
    weights = jnp.sum(jnp.where(slot == lane, lane_weights, 0.0), axis=1, keepdims=True)
    centred = []
    for c in range(3):
        taken = jnp.zeros((LIVE, LANES), F32)
        for h in range(COLUMN * CHUNKS):
            z, q = divmod(h, CHUNKS)
            row = jnp.broadcast_to(column_ref[z, c * 4 + q : c * 4 + q + 1, :], (LIVE, LANES))
            taken = jnp.where(high == h, jnp.take_along_axis(row, low, axis=1), taken)
        centred.append(taken - jnp.sum(taken, axis=1, keepdims=True) * (1.0 / TEMPLATE))
    shift = jnp.dot(
        jnp.concatenate(centred, 0),
        map_ref[...],
        precision=lax.Precision.HIGHEST,
        preferred_element_type=F32,
    )
    shift = shift * jnp.concatenate([weights] * 3, 0)
    for part in range(3):
        rounded = shift.astype(jnp.bfloat16).astype(F32)
        for c in range(3):
            shift_ref[part * 3 + c, :, :] = rounded[c * LIVE : (c + 1) * LIVE]
        shift = shift - rounded
    places = lax.broadcasted_iota(jnp.int32, (LANES, LANES), 0)
    rows = lax.broadcasted_iota(jnp.int32, (16, LANES), 0)
    total = jnp.zeros((144, LANES), F32)
    for i in range(LIVE // 4):
        lefts, rights = [], []
        for j in range(4):
            e = slice(i * 4 + j, i * 4 + j + 1)
            here = high_ref[e, :] == rows
            left = [jnp.where(here, shift_ref[n, e, :], 0.0) for n in range(9)]
            lefts.append(jnp.concatenate(left, 0).astype(jnp.bfloat16))
            rights.append(jnp.where(low_ref[e, :] == places, 1.0, 0.0).astype(jnp.bfloat16))
        total = total + lax.dot_general(
            jnp.concatenate(lefts, 1),
            jnp.concatenate(rights, 1),
            (((1,), (1,)), ((), ())),
            preferred_element_type=F32,
        )
    displaced = total[0:48] + total[48:96] + total[96:144]
    for z in range(COLUMN):
        for c in range(3):
            there = pl.ds(c * 16 + z * 4, 4)
            moved_ref[there, :] = (
                column_ref[z, c * 4 : c * 4 + 4, :] + displaced[c * 16 + z * 4 : c * 16 + z * 4 + 4]
            )
            vel_ref[there, :] = column_ref[z, 16 + c * 4 : 20 + c * 4, :]
        moved_ref[pl.ds(48 + z * 4, 4), :] = column_ref[z, 12:16, :]


def own_forces(z, source, neigh_ref, live_ref, table_ref):
    for k in range(NEIGH):
        ab, dz = divmod(k % 27, 3)
        a, b = divmod(ab, 3)
        first = ((z + dz + 3) & 3) * 4
        for c in range(4):
            for q in range(CHUNKS):
                table_ref[c, q, k : k + 1, :] = source(a, b, c, first + q)
    forces = [[None] * CHUNKS for _ in range(3)]
    for t in range(CHUNKS):
        own = [source(1, 1, c, z * 4 + t) for c in range(4)]
        total = [jnp.zeros((8, LANES), F32)] * 3
        for g in range(NEIGH // 8):
            atoms = neigh_ref[0, 0, 0, 8 * g : 8 * g + 8, t * LANES : (t + 1) * LANES]
            live = live_ref[0, 0, 0, 8 * g : 8 * g + 8, t * LANES : (t + 1) * LANES].astype(F32)
            low, high = atoms & (LANES - 1), atoms >> 7
            taken = []
            for c in range(4):
                value = jnp.take_along_axis(table_ref[c, 0, 8 * g : 8 * g + 8, :], low, axis=1)
                for q in range(1, CHUNKS):
                    other = jnp.take_along_axis(table_ref[c, q, 8 * g : 8 * g + 8, :], low, axis=1)
                    value = jnp.where(high == q, other, value)
                taken.append(value)
            apart = [own[c] - taken[c] for c in range(3)]
            square = apart[0] * apart[0] + apart[1] * apart[1] + apart[2] * apart[2]
            strength = jnp.sqrt(own[3] * taken[3]) * live
            strength = (
                strength
                * jnp.exp(-square * (0.5 / (width_scale * width_scale)))
                * (1.0 / (width_scale * width_scale))
            )
            total = [total[c] + strength * apart[c] for c in range(3)]
        for c in range(3):
            forces[c][t] = jnp.sum(total[c], axis=0, keepdims=True)
    return forces


def three_sums(forces, speeds):
    pairs = ((forces, speeds), (speeds, speeds), (forces, forces))
    lane = lax.broadcasted_iota(jnp.int32, (1, LANES), 1)
    packed = jnp.zeros((1, LANES), F32)
    for n, (left, right) in enumerate(pairs):
        added = sum(left[c][t] * right[c][t] for c in range(3) for t in range(CHUNKS))
        packed = jnp.where(lane == n, jnp.sum(added, axis=1, keepdims=True), packed)
    return packed


def read_sums(summed):
    lane = lax.broadcasted_iota(jnp.int32, (1, LANES), 1)
    return [
        jnp.sum(jnp.where(lane == n, summed, 0.0), axis=1, keepdims=True) for n in range(3)
    ]


def mix_factors(sums):
    power_sum, speed_sq, force_sq = sums
    cosine = power_sum / (jnp.sqrt(speed_sq + epsilon) * jnp.sqrt(force_sq + epsilon))
    speed_ratio = jnp.sqrt((speed_sq + epsilon) / (force_sq + epsilon))
    return 0.5 * (1.0 + cosine), mixing * speed_ratio


def new_speed(factors, speed, force):
    scale, ratio = factors
    return scale * ((1.0 - mixing) * speed + ratio * force) + time_step * force


def first_kernel(z_ref, m_ref, o_ref, p_ref, vel_ref, neigh_ref, live_ref, out_ref, table_ref):
    z = z_ref[0]
    halo = (m_ref, o_ref, p_ref)
    source = lambda a, b, c, row: halo[a][b, pl.ds(c * 16 + row, 1), :]
    forces = own_forces(z, source, neigh_ref, live_ref, table_ref)
    speeds = [
        [vel_ref[pl.ds(c * 16 + z * 4 + t, 1), :] for t in range(CHUNKS)] for c in range(3)
    ]
    sums = three_sums(forces, speeds)
    for copy in range(out_ref.shape[0]):
        for c in range(3):
            for t in range(CHUNKS):
                out_ref[copy, c * 4 + t : c * 4 + t + 1, :] = forces[c][t]
        out_ref[copy, 12:16, :] = jnp.broadcast_to(sums, (4, LANES))


def column_kernel(where_ref, parts_ref, vel_ref, out_ref, sums_ref):
    first = where_ref[1] * COLUMN
    for z in range(COLUMN):
        for c in range(3):
            out_ref[pl.ds(c * 16 + z * 4, 4), :] = parts_ref[first + z, c * 4 : c * 4 + 4, :]
    out_ref[48:96, :] = vel_ref[...]
    total = sum(parts_ref[n, 12:13, :] for n in range(parts_ref.shape[0]))
    for n in range(sums_ref.shape[0]):
        sums_ref[n, :, :] = total


def second_kernel(
    z_ref, m_ref, o_ref, p_ref, fm_ref, fo_ref, fp_ref, sums_ref, neigh_ref, live_ref,
    out_ref, own_sums_ref, table_ref, new_ref,
):
    z = z_ref[0]
    factors = mix_factors(read_sums(jnp.sum(sums_ref[...], axis=0)))
    halo, pushed = (m_ref, o_ref, p_ref), (fm_ref, fo_ref, fp_ref)
    for a in range(3):
        for b in range(3):
            speed = new_speed(factors, pushed[a][b, 48:96, :], pushed[a][b, 0:48, :])
            new_ref[a * 3 + b, 0:48, :] = halo[a][b, 0:48, :] + time_step * speed
            new_ref[a * 3 + b, 48:64, :] = halo[a][b, 48:64, :]
            if a == 1 and b == 1:
                new_ref[9, 0:48, :] = speed
    source = lambda a, b, c, row: new_ref[a * 3 + b, pl.ds(c * 16 + row, 1), :]
    forces = own_forces(z, source, neigh_ref, live_ref, table_ref)
    own = lambda n: [
        [new_ref[n, pl.ds(c * 16 + z * 4 + t, 1), :] for t in range(CHUNKS)] for c in range(3)
    ]
    places, speeds = own(4), own(9)
    for c in range(3):
        for t in range(CHUNKS):
            out_ref[c * 4 + t : c * 4 + t + 1, :] = places[c][t]
            out_ref[12 + c * 4 + t : 13 + c * 4 + t, :] = speeds[c][t]
            out_ref[24 + c * 4 + t : 25 + c * 4 + t, :] = forces[c][t]
    sums = three_sums(forces, speeds)
    for n in range(own_sums_ref.shape[0]):
        own_sums_ref[n, :, :] = sums


def final_kernel(own_ref, sums_ref, pos_ref, vel_ref):
    factors = mix_factors(read_sums(jnp.sum(sums_ref[...], axis=0)))
    speed = new_speed(factors, own_ref[12:24, :], own_ref[24:36, :])
    place = own_ref[0:12, :] + time_step * speed
    for c in range(3):
        for t in range(CHUNKS):
            cut = pl.ds(t * LANES, LANES)
            pos_ref[c, 0, 0, :, cut] = place[c * 4 + t : c * 4 + t + 1]
            vel_ref[c, 0, 0, :, cut] = speed[c * 4 + t : c * 4 + t + 1]


def exchanged(x, axes):
    return lax.all_to_all(x, axes, 0, 0, tiled=True)


def added_for_each(parts, count):
    return jnp.broadcast_to(jnp.sum(parts, 0, keepdims=True), (count, 1, LANES))


def both_sides(x, axis):
    size = lax.axis_size(axis)
    up = [(i, (i + 1) % size) for i in range(size)]
    before = lax.ppermute(x, axis, up)
    after = lax.ppermute(x, axis, [(j, i) for i, j in up])
    return before, after


def joined(before, x, after):
    row = jnp.stack([before, x, after])
    before, after = both_sides(row, GX)
    return before, row, after


def shards(
    positions,
    velocity,
    atom_eps,
    neighbours,
    pair_live,
    event_count,
    event_atoms,
    event_weight,
    template_map,
):
    x_size, y_size = lax.axis_size(GX), lax.axis_size("gy")
    z = jnp.stack([lax.axis_index("gz"), lax.axis_index("gx_1")]).astype(jnp.int32)
    inputs = (event_count, positions, velocity, atom_eps, event_weight, event_atoms)
    staged = [pltpu.VMEM(x.shape, x.dtype) for x in inputs[1:]]
    staged += [pltpu.SemaphoreType.DMA((len(staged),))]
    (own,) = call(pack_kernel, [(COLUMN, 48, LANES)], [SMEM] + [HBM] * 5, staged, None)(*inputs)
    column = exchanged(own, "gz")
    moved, speeds = call(
        events_kernel,
        [(64, LANES), (48, LANES)],
        [VMEM] * 2,
        [
            pltpu.VMEM((LIVE + EV_DEV, LANES), F32),
            pltpu.VMEM((LIVE, LANES), jnp.int32),
            pltpu.VMEM((LIVE, LANES), jnp.int32),
            pltpu.VMEM((9, LIVE, LANES), F32),
        ],
    )(column, template_map)
    before, after = both_sides(moved, "gy")
    around = joined(before, moved, after)
    table = pltpu.VMEM((4, CHUNKS, NEIGH, LANES), F32)
    (pushed,) = call(first_kernel, [(2 * COLUMN, 16, LANES)], [SMEM] + [VMEM] * 6, [table])(
        z, *around, speeds, neighbours, pair_live
    )
    pushed = exchanged(pushed, CORE_Z)
    forces, sums = call(
        column_kernel, [(96, LANES), (x_size // 2 * y_size, 1, LANES)], [SMEM] + [VMEM] * 2
    )(z, pushed, speeds)
    before, after = both_sides(forces, "gy")
    sums = exchanged(sums, X_Y)
    forces_around = joined(before, forces, after)
    result, sums = call(
        second_kernel,
        [(40, LANES), (x_size * COLUMN, 1, LANES)],
        [SMEM] + [VMEM] * 9,
        [table, pltpu.VMEM((10, 64, LANES), F32)],
    )(z, *around, *forces_around, sums, neighbours, pair_live)
    sums = exchanged(sums, GXZ)
    sums = exchanged(added_for_each(sums, y_size), "gy")
    return tuple(
        call(final_kernel, [positions.shape, velocity.shape], [VMEM] * 2)(result, sums)
    )


def solution(mesh):
    shape = mesh.shape
    split = Mesh(
        mesh.devices.reshape(shape["gx"] // 2, 2, shape["gy"], shape["gz"]),
        ("gx_0", "gx_1", "gy", "gz"),
    )
    in_specs = (
        P(None, GX, "gy", "gz", None),
        P(None, GX, "gy", "gz", None),
        P(GX, "gy", "gz", None),
        P(GX, "gy", "gz", None, None),
        P(GX, "gy", "gz", None, None),
        P(GX, "gy", "gz"),
        P(GX, "gy", "gz", None, None),
        P(GX, "gy", "gz", None),
        P(),
    )
    out_specs = (P(None, GX, "gy", "gz", None), P(None, GX, "gy", "gz", None))
    return jax.shard_map(
        shards, mesh=split, in_specs=in_specs, out_specs=out_specs, check_vma=False
    )
```

```python
import jax
import jax.numpy as jnp
from jax import lax
from jax.experimental import pallas as pl
from jax.experimental.pallas import tpu as pltpu
from jax.sharding import Mesh
from jax.sharding import PartitionSpec as P

EV_DEV = 16
NEIGH = 32
TEMPLATE = 128
GX = ("gx_0", "gx_1")
GXZ = ("gx_0", "gx_1", "gz")
X_Y = ("gx_0", "gy")
CORE_Z = ("gx_1", "gz")
COLUMN = 4
CHUNKS = 4
LIVE = 32
LANES = 128
F32 = jnp.float32

width_scale = 1.5
time_step = 0.1
mixing = 0.1
epsilon = 1e-06

SMEM = pl.BlockSpec(memory_space=pltpu.SMEM)
VMEM = pl.BlockSpec(memory_space=pltpu.VMEM)
HBM = pl.BlockSpec(memory_space=pltpu.HBM)


def call(kernel, outs, specs, scratch=(), limit=4 << 20):
    return pl.pallas_call(
        kernel,
        out_shape=[jax.ShapeDtypeStruct(shape, F32) for shape in outs],
        in_specs=specs,
        out_specs=[VMEM] * len(outs),
        scratch_shapes=list(scratch),
        cost_estimate=pl.CostEstimate(flops=10000, bytes_accessed=100000, transcendentals=0),
        compiler_params=pltpu.CompilerParams(vmem_limit_bytes=limit),
    )


def pack_kernel(
    count_ref, pos_hbm, vel_hbm, eps_hbm, weight_hbm, atoms_hbm, out_ref,
    pos_ref, vel_ref, eps_ref, weight_ref, atoms_ref, sems,
):
    pairs = (
        (pos_hbm, pos_ref),
        (vel_hbm, vel_ref),
        (eps_hbm, eps_ref),
        (weight_hbm, weight_ref),
        (atoms_hbm, atoms_ref),
    )
    copies = [pltpu.make_async_copy(*pair, sems.at[n]) for n, pair in enumerate(pairs)]
    for copy in copies:
        copy.start()
    for copy in range(COLUMN):
        out_ref[copy, 24:32, :] = jnp.zeros((8, LANES), F32)
    for copy in copies:
        copy.wait()
    count = count_ref[0, 0, 0]
    live = lax.broadcasted_iota(jnp.int32, (1, EV_DEV), 1) < count
    weights = jnp.where(live, weight_ref[0, 0, :, :], 0.0)
    counts = jnp.full((1, LANES), count, jnp.int32).astype(F32)
    atoms = atoms_ref[0, 0, 0, :, :].astype(F32)
    for copy in range(COLUMN):
        for c in range(3):
            for q in range(CHUNKS):
                cut = pl.ds(q * LANES, LANES)
                out_ref[copy, c * 4 + q : c * 4 + q + 1, :] = pos_ref[c, 0, 0, :, cut]
                out_ref[copy, 16 + c * 4 + q : 17 + c * 4 + q, :] = vel_ref[c, 0, 0, :, cut]
        for q in range(CHUNKS):
            out_ref[copy, 12 + q : 13 + q, :] = eps_ref[0, 0, :, pl.ds(q * LANES, LANES)]
        out_ref[copy, 28:29, 0:EV_DEV] = weights
        out_ref[copy, 29:30, :] = counts
        out_ref[copy, 32:48, :] = atoms


def events_kernel(column_ref, map_ref, moved_ref, vel_ref, atoms_ref, low_ref, high_ref, shift_ref):
    atoms_ref[...] = jnp.zeros(atoms_ref.shape, F32)
    first = jnp.int32(0)
    lane_weights = jnp.zeros((1, LANES), F32)
    for z in range(COLUMN):
        for e in range(EV_DEV):
            atoms_ref[pl.ds(first + e, 1), :] = column_ref[z, 32 + e : 33 + e, :]
        lane_weights = lane_weights + pltpu.roll(column_ref[z, 28:29, :], first, 1)
        if z < COLUMN - 1:
            first = first + jnp.max(column_ref[z, 29:30, :]).astype(jnp.int32)
    atoms = atoms_ref[0:LIVE, :].astype(jnp.int32)
    low, high = atoms & (LANES - 1), atoms >> 7
    low_ref[...] = low
    high_ref[...] = high
    slot = lax.broadcasted_iota(jnp.int32, (LIVE, LANES), 0)
    lane = lax.broadcasted_iota(jnp.int32, (LIVE, LANES), 1)
    weights = jnp.sum(jnp.where(slot == lane, lane_weights, 0.0), axis=1, keepdims=True)
    centred = []
    for c in range(3):
        taken = jnp.zeros((LIVE, LANES), F32)
        for h in range(COLUMN * CHUNKS):
            z, q = divmod(h, CHUNKS)
            row = jnp.broadcast_to(column_ref[z, c * 4 + q : c * 4 + q + 1, :], (LIVE, LANES))
            taken = jnp.where(high == h, jnp.take_along_axis(row, low, axis=1), taken)
        centred.append(taken - jnp.sum(taken, axis=1, keepdims=True) * (1.0 / TEMPLATE))
    shift = jnp.dot(
        jnp.concatenate(centred, 0),
        map_ref[...],
        precision=lax.Precision.HIGHEST,
        preferred_element_type=F32,
    )
    shift = shift * jnp.concatenate([weights] * 3, 0)
    for part in range(3):
        rounded = shift.astype(jnp.bfloat16).astype(F32)
        for c in range(3):
            shift_ref[part * 3 + c, :, :] = rounded[c * LIVE : (c + 1) * LIVE]
        shift = shift - rounded
    places = lax.broadcasted_iota(jnp.int32, (LANES, LANES), 0)
    rows = lax.broadcasted_iota(jnp.int32, (16, LANES), 0)
    total = jnp.zeros((144, LANES), F32)
    for i in range(LIVE // 4):
        lefts, rights = [], []
        for j in range(4):
            e = slice(i * 4 + j, i * 4 + j + 1)
            here = high_ref[e, :] == rows
            left = [jnp.where(here, shift_ref[n, e, :], 0.0) for n in range(9)]
            lefts.append(jnp.concatenate(left, 0).astype(jnp.bfloat16))
            rights.append(jnp.where(low_ref[e, :] == places, 1.0, 0.0).astype(jnp.bfloat16))
        total = total + lax.dot_general(
            jnp.concatenate(lefts, 1),
            jnp.concatenate(rights, 1),
            (((1,), (1,)), ((), ())),
            preferred_element_type=F32,
        )
    displaced = total[0:48] + total[48:96] + total[96:144]
    for z in range(COLUMN):
        for c in range(3):
            there = pl.ds(c * 16 + z * 4, 4)
            moved_ref[there, :] = (
                column_ref[z, c * 4 : c * 4 + 4, :] + displaced[c * 16 + z * 4 : c * 16 + z * 4 + 4]
            )
            vel_ref[there, :] = column_ref[z, 16 + c * 4 : 20 + c * 4, :]
        moved_ref[pl.ds(48 + z * 4, 4), :] = column_ref[z, 12:16, :]


def own_forces(z, source, neigh_ref, live_ref, table_ref):
    for k in range(NEIGH):
        ab, dz = divmod(k % 27, 3)
        a, b = divmod(ab, 3)
        first = ((z + dz + 3) & 3) * 4
        for c in range(4):
            for q in range(CHUNKS):
                table_ref[c, q, k : k + 1, :] = source(a, b, c, first + q)
    forces = [[None] * CHUNKS for _ in range(3)]
    for t in range(CHUNKS):
        own = [source(1, 1, c, z * 4 + t) for c in range(4)]
        total = [jnp.zeros((8, LANES), F32)] * 3
        for g in range(NEIGH // 8):
            atoms = neigh_ref[0, 0, 0, 8 * g : 8 * g + 8, t * LANES : (t + 1) * LANES]
            live = live_ref[0, 0, 0, 8 * g : 8 * g + 8, t * LANES : (t + 1) * LANES].astype(F32)
            low, high = atoms & (LANES - 1), atoms >> 7
            taken = []
            for c in range(4):
                value = jnp.take_along_axis(table_ref[c, 0, 8 * g : 8 * g + 8, :], low, axis=1)
                for q in range(1, CHUNKS):
                    other = jnp.take_along_axis(table_ref[c, q, 8 * g : 8 * g + 8, :], low, axis=1)
                    value = jnp.where(high == q, other, value)
                taken.append(value)
            apart = [own[c] - taken[c] for c in range(3)]
            square = apart[0] * apart[0] + apart[1] * apart[1] + apart[2] * apart[2]
            strength = jnp.sqrt(own[3] * taken[3]) * live
            strength = (
                strength
                * jnp.exp(-square * (0.5 / (width_scale * width_scale)))
                * (1.0 / (width_scale * width_scale))
            )
            total = [total[c] + strength * apart[c] for c in range(3)]
        for c in range(3):
            forces[c][t] = jnp.sum(total[c], axis=0, keepdims=True)
    return forces


def three_sums(forces, speeds):
    pairs = ((forces, speeds), (speeds, speeds), (forces, forces))
    lane = lax.broadcasted_iota(jnp.int32, (1, LANES), 1)
    packed = jnp.zeros((1, LANES), F32)
    for n, (left, right) in enumerate(pairs):
        added = sum(left[c][t] * right[c][t] for c in range(3) for t in range(CHUNKS))
        packed = jnp.where(lane == n, jnp.sum(added, axis=1, keepdims=True), packed)
    return packed


def read_sums(summed):
    lane = lax.broadcasted_iota(jnp.int32, (1, LANES), 1)
    return [
        jnp.sum(jnp.where(lane == n, summed, 0.0), axis=1, keepdims=True) for n in range(3)
    ]


def mix_factors(sums):
    power_sum, speed_sq, force_sq = sums
    cosine = power_sum / (jnp.sqrt(speed_sq + epsilon) * jnp.sqrt(force_sq + epsilon))
    speed_ratio = jnp.sqrt((speed_sq + epsilon) / (force_sq + epsilon))
    return 0.5 * (1.0 + cosine), mixing * speed_ratio


def new_speed(factors, speed, force):
    scale, ratio = factors
    return scale * ((1.0 - mixing) * speed + ratio * force) + time_step * force


def first_kernel(z_ref, m_ref, o_ref, p_ref, vel_ref, neigh_ref, live_ref, out_ref, table_ref):
    z = z_ref[0] & (COLUMN - 1)
    halo = (m_ref, o_ref, p_ref)
    source = lambda a, b, c, row: halo[a][b, pl.ds(c * 16 + row, 1), :]
    forces = own_forces(z, source, neigh_ref, live_ref, table_ref)
    speeds = [
        [vel_ref[pl.ds(c * 16 + z * 4 + t, 1), :] for t in range(CHUNKS)] for c in range(3)
    ]
    sums = three_sums(forces, speeds)
    for copy in range(out_ref.shape[0]):
        for c in range(3):
            for t in range(CHUNKS):
                out_ref[copy, c * 4 + t : c * 4 + t + 1, :] = forces[c][t]
        out_ref[copy, 12:16, :] = jnp.broadcast_to(sums, (4, LANES))


def column_kernel(where_ref, parts_ref, vel_ref, out_ref, sums_ref):
    first = where_ref[0] & COLUMN
    for z in range(COLUMN):
        for c in range(3):
            out_ref[pl.ds(c * 16 + z * 4, 4), :] = parts_ref[first + z, c * 4 : c * 4 + 4, :]
    out_ref[48:96, :] = vel_ref[...]
    total = sum(parts_ref[n, 12:13, :] for n in range(parts_ref.shape[0]))
    for n in range(sums_ref.shape[0]):
        sums_ref[n, :, :] = total


def second_kernel(
    z_ref, m_ref, o_ref, p_ref, fm_ref, fo_ref, fp_ref, sums_ref, neigh_ref, live_ref,
    out_ref, own_sums_ref, table_ref, new_ref,
):
    z = z_ref[0] & (COLUMN - 1)
    factors = mix_factors(read_sums(sums_ref[...]))
    halo, pushed = (m_ref, o_ref, p_ref), (fm_ref, fo_ref, fp_ref)
    for a in range(3):
        for b in range(3):
            speed = new_speed(factors, pushed[a][b, 48:96, :], pushed[a][b, 0:48, :])
            new_ref[a * 3 + b, 0:48, :] = halo[a][b, 0:48, :] + time_step * speed
            new_ref[a * 3 + b, 48:64, :] = halo[a][b, 48:64, :]
            if a == 1 and b == 1:
                new_ref[9, 0:48, :] = speed
    source = lambda a, b, c, row: new_ref[a * 3 + b, pl.ds(c * 16 + row, 1), :]
    forces = own_forces(z, source, neigh_ref, live_ref, table_ref)
    own = lambda n: [
        [new_ref[n, pl.ds(c * 16 + z * 4 + t, 1), :] for t in range(CHUNKS)] for c in range(3)
    ]
    places, speeds = own(4), own(9)
    for c in range(3):
        for t in range(CHUNKS):
            out_ref[c * 4 + t : c * 4 + t + 1, :] = places[c][t]
            out_ref[12 + c * 4 + t : 13 + c * 4 + t, :] = speeds[c][t]
            out_ref[24 + c * 4 + t : 25 + c * 4 + t, :] = forces[c][t]
    sums = three_sums(forces, speeds)
    for n in range(own_sums_ref.shape[0]):
        own_sums_ref[n, :, :] = sums


def final_kernel(own_ref, sums_ref, pos_ref, vel_ref):
    factors = mix_factors(read_sums(jnp.sum(sums_ref[...], axis=0)))
    speed = new_speed(factors, own_ref[12:24, :], own_ref[24:36, :])
    place = own_ref[0:12, :] + time_step * speed
    for c in range(3):
        for t in range(CHUNKS):
            cut = pl.ds(t * LANES, LANES)
            pos_ref[c, 0, 0, :, cut] = place[c * 4 + t : c * 4 + t + 1]
            vel_ref[c, 0, 0, :, cut] = speed[c * 4 + t : c * 4 + t + 1]


def exchanged(x, axes):
    return lax.all_to_all(x, axes, 0, 0, tiled=True)


def added_for_each(parts, count):
    return jnp.broadcast_to(jnp.sum(parts, 0, keepdims=True), (count, 1, LANES))


def both_sides(x, axis):
    size = lax.axis_size(axis)
    up = [(i, (i + 1) % size) for i in range(size)]
    before = lax.ppermute(x, axis, up)
    after = lax.ppermute(x, axis, [(j, i) for i, j in up])
    return before, after


def joined(before, x, after):
    row = jnp.stack([before, x, after])
    before, after = both_sides(row, GX)
    return before, row, after


def shards(
    positions,
    velocity,
    atom_eps,
    neighbours,
    pair_live,
    event_count,
    event_atoms,
    event_weight,
    template_map,
):
    x_size, y_size = lax.axis_size(GX), lax.axis_size("gy")
    z = (lax.axis_index("gz") + COLUMN * lax.axis_index("gx_1")).astype(jnp.int32).reshape(1)
    inputs = (event_count, positions, velocity, atom_eps, event_weight, event_atoms)
    staged = [pltpu.VMEM(x.shape, x.dtype) for x in inputs[1:]]
    staged += [pltpu.SemaphoreType.DMA((len(staged),))]
    (own,) = call(pack_kernel, [(COLUMN, 48, LANES)], [SMEM] + [HBM] * 5, staged, None)(*inputs)
    column = exchanged(own, "gz")
    moved, speeds = call(
        events_kernel,
        [(64, LANES), (48, LANES)],
        [VMEM] * 2,
        [
            pltpu.VMEM((LIVE + EV_DEV, LANES), F32),
            pltpu.VMEM((LIVE, LANES), jnp.int32),
            pltpu.VMEM((LIVE, LANES), jnp.int32),
            pltpu.VMEM((9, LIVE, LANES), F32),
        ],
    )(column, template_map)
    before, after = both_sides(moved, "gy")
    around = joined(before, moved, after)
    table = pltpu.VMEM((4, CHUNKS, NEIGH, LANES), F32)
    (pushed,) = call(first_kernel, [(2 * COLUMN, 16, LANES)], [SMEM] + [VMEM] * 6, [table])(
        z, *around, speeds, neighbours, pair_live
    )
    pushed = exchanged(pushed, CORE_Z)
    forces, sums = call(
        column_kernel, [(96, LANES), (x_size // 2 * y_size, 1, LANES)], [SMEM] + [VMEM] * 2
    )(z, pushed, speeds)
    before, after = both_sides(forces, "gy")
    forces_around = joined(before, forces, after)
    sums = jnp.sum(exchanged(sums, X_Y), 0)
    result, sums = call(
        second_kernel,
        [(40, LANES), (x_size * COLUMN, 1, LANES)],
        [SMEM] + [VMEM] * 9,
        [table, pltpu.VMEM((10, 64, LANES), F32)],
    )(z, *around, *forces_around, sums, neighbours, pair_live)
    sums = exchanged(sums, GXZ)
    sums = exchanged(added_for_each(sums, y_size), "gy")
    return tuple(
        call(final_kernel, [positions.shape, velocity.shape], [VMEM] * 2)(result, sums)
    )


def solution(mesh):
    shape = mesh.shape
    split = Mesh(
        mesh.devices.reshape(shape["gx"] // 2, 2, shape["gy"], shape["gz"]),
        ("gx_0", "gx_1", "gy", "gz"),
    )
    in_specs = (
        P(None, GX, "gy", "gz", None),
        P(None, GX, "gy", "gz", None),
        P(GX, "gy", "gz", None),
        P(GX, "gy", "gz", None, None),
        P(GX, "gy", "gz", None, None),
        P(GX, "gy", "gz"),
        P(GX, "gy", "gz", None, None),
        P(GX, "gy", "gz", None),
        P(),
    )
    out_specs = (P(None, GX, "gy", "gz", None), P(None, GX, "gy", "gz", None))
    return jax.shard_map(
        shards, mesh=split, in_specs=in_specs, out_specs=out_specs, check_vma=False
    )
```
